128 devices in a mesh: cp: 8 (over z, y_lo), tp: 16 (over x, y_hi, core).
Axes of the slice: x: 4, y: 4 (y_hi: 2, y_lo: 2; y = y_hi * 2 + y_lo), z: 4, core: 2. Of those that a mesh axis runs over, the one named last changes fastest.
Arguments:
- checkpoint: bfloat16 [4096, 8192], P('cp', 'tp'), may hold values from -6 to 6
- norm_gain: float32 [8192], replicated, may hold values from 0.1 to 1.9
- query_weight: bfloat16 [8192, 8192], P(None, 'tp'), may hold values from -4 to 4
- key_weight: bfloat16 [8192, 1024], P(None, 'tp'), may hold values from -1 to 1
- value_weight: bfloat16 [8192, 1024], P(None, 'tp'), may hold values from -0.0625 to 0.0625
- output_weight: bfloat16 [8192, 8192], P('tp'), may hold values from -0.09375 to 0.09375
- block_order: int32 [16], replicated, may hold values from 0 to 15, each once
Outputs:
- projected: bfloat16 [4096, 8192], P('cp', 'tp')
- log_normalizer: float32 [64, 4096], P('tp', 'cp')
The draws below stay inside these ranges and needn't reach their ends.
Inputs may be any that keep to these rules, and one draw needn't show every extreme that they name: `block_order`: each of 0 to 15 once.
All inputs are finite; a program needn't handle non-finite values.
Results may differ from the reference program's by a relative error of at most 0.019.
Values may be sent and summed in bfloat16 or wider, within the bound.
A program may use at most 128 MiB of HBM per device.

```python
import math
import jax
import jax.numpy as jnp
from jax import lax

D = 8192
HEADS = 64
KV_HEADS = 8
HEAD_DIM = 128
SEQ = 4096
BLOCK = 256
N_CP = 8
N_TP = 16


def joint_query_key(key):
    shared_keys = jax.random.normal(jax.random.fold_in(key, 17), (D, KV_HEADS * HEAD_DIM), jnp.float32) / math.sqrt(D)
    shared_keys = jnp.clip(shared_keys, -1.0, 1.0)
    queries = jax.random.normal(jax.random.fold_in(key, 29), (D, HEADS * HEAD_DIM), jnp.float32) * (2.5 / math.sqrt(D))
    queries = jnp.clip(queries, -4.0, 4.0)
    return (queries, shared_keys)


def draw_query_weight(key, part):
    return joint_query_key(key)[0].astype(jnp.bfloat16)


def draw_key_weight(key, part):
    return joint_query_key(key)[1].astype(jnp.bfloat16)


def raised(values, stream_key, source, target, parts, factor):
    def block_of(axis_at):
        return (jnp.arange(values.shape[axis_at]) // (values.shape[axis_at] // parts)).reshape((-1,) + (1,) * (values.ndim - 1 - axis_at))

    first = jax.random.permutation(stream_key, parts)[block_of(target)]
    second = (block_of(target) + parts // 2) % parts
    return jnp.where((block_of(source) == first) | (block_of(source) == second), factor * values, values)


def steps_of(rng, dims, cuts, smallest, largest):
    def one(dim, blocks):
        steps = jax.random.uniform(jax.random.fold_in(jax.random.fold_in(rng, 6), dim), (blocks,), jnp.float32, smallest / len(cuts), largest / len(cuts))
        return jnp.repeat(jnp.exp(steps), dims[dim] // blocks).reshape((-1,) + (1,) * (len(dims) - dim - 1))

    gain = one(*cuts[0])
    for cut in cuts[1:]:
        gain = gain * one(*cut)
    return gain


def scatter_about(own_key, dims, spread, limit, shards=(), held_as=jnp.bfloat16):
    result = spread * jax.random.normal(own_key, dims, jnp.float32)
    if shards:
        result = result * steps_of(own_key, dims, shards, -0.22, 0.18)
    return jnp.clip(result, -limit, limit).astype(held_as)


def heavy_noise(own_key, shape, spread, limit, cuts, heavy, kind=jnp.bfloat16):
    entries = spread * jax.random.normal(own_key, shape, jnp.float32)
    if cuts:
        entries = entries * steps_of(own_key, shape, cuts, -0.22, 0.18)
    return jnp.clip(raised(entries, jax.random.fold_in(own_key, 3), *heavy), -limit, limit).astype(kind)


def setup_inputs(seed: int = 0) -> dict:
    streams_of = jax.random.split(jax.random.key(seed), 8)
    checkpoint = scatter_about(streams_of[0], (SEQ, D), 1.0, 6.0, ((0, 8), (1, 16)))
    norm_gain = jnp.clip(1.0 + 0.18 * jax.random.normal(streams_of[1], (D,), jnp.float32), 0.1, 1.9)
    query_weight = draw_query_weight(jax.random.fold_in(streams_of[7], 71), 0)
    key_weight = draw_key_weight(jax.random.fold_in(streams_of[7], 71), 0)
    value_weight = scatter_about(streams_of[4], (D, KV_HEADS * HEAD_DIM), D ** -0.5, 0.0625, ((1, 16),))
    output_weight = heavy_noise(streams_of[5], (HEADS * HEAD_DIM, D), (HEADS * HEAD_DIM) ** -0.5, 0.09375, ((0, 16),), (0, 1, 16, 2.0))
    block_order = jax.random.permutation(streams_of[6], 2 * N_CP).astype(jnp.int32)
    return {"checkpoint": checkpoint, "norm_gain": norm_gain, "query_weight": query_weight, "key_weight": key_weight, "value_weight": value_weight, "output_weight": output_weight, "block_order": block_order}


rope_base = 500000.0
norm_epsilon = 1e-05

def turn_pairs(matrix, positions, first_pair):
    pair_count = matrix.shape[-1] // 2
    pair_index = (first_pair + jnp.arange(pair_count, dtype=jnp.int32)).astype(jnp.float32)
    inverse_rates = rope_base ** (-2.0 * pair_index / HEAD_DIM)
    angles = positions.astype(jnp.float32)[:, None] * inverse_rates[None, :]
    cosine = jnp.cos(angles)[:, None, :]
    sine_part = jnp.sin(angles)[:, None, :]
    paired = matrix.reshape(matrix.shape[0], matrix.shape[1], pair_count, 2)
    former = paired[..., 0]
    latter = paired[..., 1]
    turned = jnp.stack([former * cosine - latter * sine_part, former * sine_part + latter * cosine], axis=-1)
    return turned.reshape(matrix.shape)

def reference(checkpoint, norm_gain, query_weight, key_weight, value_weight, output_weight, block_order):
    seq_rows = jnp.arange(SEQ, dtype=jnp.int32)
    positions = (block_order[seq_rows // BLOCK] * BLOCK + seq_rows % BLOCK).astype(jnp.int32)
    widened = checkpoint.astype(jnp.float32)
    mean_square = lax.optimization_barrier(jnp.mean(widened * widened, axis=-1, keepdims=True))
    normed = (widened * lax.rsqrt(mean_square + norm_epsilon) * norm_gain).astype(jnp.bfloat16)
    query_features = jnp.dot(normed, query_weight, preferred_element_type=jnp.float32)
    key_features = jnp.dot(normed, key_weight, preferred_element_type=jnp.float32)
    value_features = jnp.dot(normed, value_weight, preferred_element_type=jnp.float32)
    queries = turn_pairs(query_features.reshape(SEQ, HEADS, HEAD_DIM), positions, 0).astype(jnp.bfloat16)
    keys = turn_pairs(key_features.reshape(SEQ, KV_HEADS, HEAD_DIM), positions, 0).astype(jnp.bfloat16)
    values = value_features.astype(jnp.bfloat16).reshape(SEQ, KV_HEADS, HEAD_DIM)
    by_head_queries = jnp.transpose(queries, (1, 0, 2))
    key_heads = jnp.transpose(keys, (1, 0, 2))
    value_heads = jnp.transpose(values, (1, 0, 2))
    group_size = HEADS // KV_HEADS
    allowed = positions[None, :] <= positions[:, None]
    score_scale = 1.0 / math.sqrt(HEAD_DIM)

    def one_head(head_index):
        query_block = lax.dynamic_index_in_dim(by_head_queries, head_index, 0, keepdims=False)
        key_block = lax.dynamic_index_in_dim(key_heads, head_index // group_size, 0, keepdims=False)
        value_block = lax.dynamic_index_in_dim(value_heads, head_index // group_size, 0, keepdims=False)
        scores = jnp.dot(query_block, key_block.T, preferred_element_type=jnp.float32) * score_scale
        scores = jnp.where(allowed, scores, -jnp.inf)
        row_top = lax.optimization_barrier(jnp.max(scores, axis=-1, keepdims=True))
        normalizer = row_top + jnp.log(lax.optimization_barrier(jnp.sum(jnp.exp(scores - row_top), axis=-1, keepdims=True)))
        weights = jnp.exp(scores - normalizer).astype(jnp.bfloat16)
        attended_head = jnp.dot(weights, value_block, preferred_element_type=jnp.float32).astype(jnp.bfloat16)
        return (attended_head, normalizer[:, 0])
    attended, log_normalizer = lax.map(one_head, jnp.arange(HEADS, dtype=jnp.int32))
    attended_flat = jnp.transpose(attended, (1, 0, 2)).reshape(SEQ, HEADS * HEAD_DIM)
    group_rows = HEADS * HEAD_DIM // N_TP
    attended_groups = jnp.transpose(attended_flat.reshape(SEQ, N_TP, group_rows), (1, 0, 2))
    weight_groups = output_weight.reshape(N_TP, group_rows, D)

    def add_group(running_total, pieces):
        group_term = jnp.dot(pieces[0], pieces[1], preferred_element_type=jnp.float32).astype(jnp.bfloat16)
        group_term = lax.optimization_barrier(group_term)
        return (running_total + group_term.astype(jnp.float32), None)
    running_total, unused = lax.scan(add_group, jnp.zeros((SEQ, D), jnp.float32), (attended_groups, weight_groups))
    return (running_total.astype(jnp.bfloat16), log_normalizer)
```

```python
import functools
import math

import jax
import jax.numpy as jnp
from jax import lax
from jax.experimental import pallas as pl
from jax.experimental.pallas import tpu as pltpu
from jax.sharding import PartitionSpec as P

MESH = pl.DeviceIdType.MESH
HEAD = 128
ROWS = 256
FEAT = 512
HALF = ROWS // 2
N_TP = 16
N_CP = 8
D = 8192
rope_base = 500000.0
norm_epsilon = 1e-05
masked_score = -1e30
LN2 = math.log(2.0)

f32 = jnp.float32
bf16 = jnp.bfloat16


def pick(i, values):
    out = values[-1]
    for n in range(len(values) - 2, -1, -1):
        out = jnp.where(i == n, values[n], out)
    return out


class Gather:
    def __init__(self, slot, ssem, rsem, right, left, pair, core):
        self.slot, self.ssem, self.rsem = slot, ssem, rsem
        self.right, self.left, self.pair, self.core = right, left, pair, core
        self.blocks = [(0, 0), (3, 0), (1, 0), (2, 0), (0, 1), (3, 1), (1, 1), (2, 1)]

    def ref(self, c, dr, dp, dk=0, rows=None):
        ref = self.slot(c, dr, dp, dk)
        return ref if rows is None else ref.at[pl.ds(rows * HALF, HALF)]

    def copy(self, c, n, ref, device):
        return pltpu.make_async_remote_copy(
            src_ref=ref,
            dst_ref=ref,
            send_sem=self.ssem.at[c * 17 + n],
            recv_sem=self.rsem.at[c * 17 + n],
            device_id=device,
            device_id_type=MESH,
        )

    def send_core(self, c, b):
        self.copy(c, 9 + b, self.ref(c, *self.blocks[b]), self.core).start()

    def start(self, c):
        own = self.ref(c, 0, 0)
        self.copy(c, 8, own, self.pair).start()
        self.copy(c, 0, own, self.right).start()
        self.copy(c, 4, own, self.left).start()
        self.send_core(c, 0)

    def from_left(self, c, dp):
        self.copy(c, 2 * dp, self.ref(c, 3, dp), self.left).wait_recv()
        self.copy(c, 1 + 2 * dp, self.ref(c, 3, dp, rows=0), self.right).start()
        self.send_core(c, 1 + 4 * dp)

    def from_right(self, c, dp):
        self.copy(c, 4 + 2 * dp, self.ref(c, 1, dp), self.right).wait_recv()
        self.copy(c, 5 + 2 * dp, self.ref(c, 1, dp, rows=1), self.left).start()
        self.send_core(c, 2 + 4 * dp)

    def from_pair(self, c):
        block = self.ref(c, 0, 1)
        self.copy(c, 8, block, self.pair).wait_recv()
        self.copy(c, 2, block, self.right).start()
        self.copy(c, 6, block, self.left).start()
        self.send_core(c, 4)

    def from_far(self, c, dp):
        self.copy(c, 1 + 2 * dp, self.ref(c, 2, dp, rows=0), self.left).wait_recv()
        self.copy(c, 5 + 2 * dp, self.ref(c, 2, dp, rows=1), self.right).wait_recv()
        self.send_core(c, 3 + 4 * dp)

    def from_core(self, c, b):
        self.copy(c, 9 + b, self.ref(c, *self.blocks[b], dk=1), self.core).wait_recv()

    def drain(self, c):
        for n in range(17):
            half = n in (1, 3, 5, 7)
            ref = self.ref(c, 0, 0, rows=0 if half else None)
            self.copy(c, n, ref, self.core).wait_send()


def kernel(
    order, x_hbm, gain, cq, sq, ck, sk, wq_hbm, wkv_hbm, wo_hbm,
    proj, norm_out,
    xg, wq, wkv, wo, acc, ss, q, kvg, kt, v1, scr, top, outs, att, bias,
    ro, ra, rb, rc, rd, ry,
    x_sem, w_sem, wo_sem, gs, gr, ks, kr, rs, rr,
):
    tp, cp = lax.axis_index("tp"), lax.axis_index("cp")
    core, yh, xx = tp % 2, (tp // 2) % 2, tp // 4
    yl, zz = cp % 2, cp // 2

    def tpi(dr, dp, dk):
        return (((xx + dr) % 4) * 2 + (yh + dp) % 2) * 2 + (core + dk) % 2

    def cpi(dr, dp):
        return ((zz + dr) % 4) * 2 + (yl + dp) % 2

    right, left = {"tp": tpi(1, 0, 0)}, {"tp": tpi(3, 0, 0)}
    pair, other = {"tp": tpi(0, 1, 0)}, {"tp": tpi(0, 0, 1)}
    up, down, beside = {"cp": cpi(1, 0)}, {"cp": cpi(3, 0)}, {"cp": cpi(0, 1)}

    dr_of = (0, 0, 3, 1, 3, 1, 2, 2)
    dk_of = (0, 1, 0, 0, 1, 1, 0, 1)

    def slot_at(i):
        return tpi(pick(i % 8, dr_of), i // 8, pick(i % 8, dk_of))

    x_copies = [
        pltpu.make_async_copy(x_hbm.at[pl.ds(c * ROWS, ROWS)], xg.at[c, tp], x_sem.at[c])
        for c in range(2)
    ]
    for copy in x_copies:
        copy.start()

    def w_copies(i):
        rows = pl.ds(pl.multiple_of(slot_at(i) * FEAT, FEAT), FEAT)
        return (
            pltpu.make_async_copy(wq_hbm.at[rows], wq.at[rows], w_sem.at[i]),
            pltpu.make_async_copy(wkv_hbm.at[rows], wkv.at[rows], w_sem.at[16 + i]),
        )

    for i in range(16):
        for copy in w_copies(i):
            copy.start()
    wo_copy = pltpu.make_async_copy(wo_hbm, wo, wo_sem)
    wo_copy.start()

    barrier = pltpu.get_barrier_semaphore()
    neighbours = (right, left, pair, other, up, down, beside)
    for device in neighbours:
        pl.semaphore_signal(barrier, inc=1, device_id=device, device_id_type=MESH)
    pl.semaphore_wait(barrier, len(neighbours))

    g = Gather(lambda c, dr, dp, dk: xg.at[c, tpi(dr, dp, dk)], gs, gr, right, left, pair, other)
    kv = Gather(
        lambda c, dr, dp, dk: kvg.at[c, (core + dk) % 2, cpi(dr, dp)], ks, kr, up, down, beside, other
    )

    for c in range(2):
        x_copies[c].wait()
        g.start(c)

    row_id = lax.broadcasted_iota(jnp.int32, (ROWS, ROWS), 0)
    col_id = lax.broadcasted_iota(jnp.int32, (ROWS, ROWS), 1)
    bias[0] = jnp.zeros((ROWS, ROWS), f32)
    bias[1] = jnp.where(col_id <= row_id, 0.0, masked_score).astype(f32)
    bias[2] = jnp.full((ROWS, ROWS), masked_score, f32)
    acc[...] = jnp.zeros_like(acc)
    ss[...] = jnp.zeros_like(ss)

    def project(c, i):
        j = slot_at(i)
        wide = xg[c, j].astype(f32)
        square = wide * wide
        ss[c] += square[:, :128] + square[:, 128:256] + square[:, 256:384] + square[:, 384:]
        scaled = (wide * gain[pl.ds(j, 1), :]).astype(bf16)
        rows = pl.ds(pl.multiple_of(j * FEAT, FEAT), FEAT)
        acc[c, :, :FEAT] += jnp.dot(scaled, wq[rows, :], preferred_element_type=f32)
        acc[c, :, FEAT:] += jnp.dot(scaled, wkv[rows, :], preferred_element_type=f32)

    even = (lax.broadcasted_iota(jnp.int32, (ROWS, HEAD), 1) % 2) == 0

    def turn(y, cosine, sine):
        swapped = jnp.where(even, pltpu.roll(y, HEAD - 1, 1), pltpu.roll(y, 1, 1))
        return y * cosine + swapped * sine

    def finish(c):
        scale = lax.rsqrt(jnp.sum(ss[c], axis=1, keepdims=True) * (1.0 / D) + norm_epsilon)
        scale = jnp.broadcast_to(scale, (ROWS, HEAD))
        part = slice(c * ROWS, (c + 1) * ROWS)
        kvg[c, core, cp] = turn(acc[c, :, FEAT:] * scale, ck[part], sk[part]).astype(bf16)
        kv.start(c)
        for h in range(4):
            y = acc[c, :, h * HEAD : (h + 1) * HEAD] * scale
            q[c, h] = turn(y, cq[part], sq[part]).astype(bf16)

    def assemble(c, s):
        lower, upper = kvg[c, 0, s].astype(f32), kvg[c, 1, s].astype(f32)
        low = lax.broadcasted_iota(jnp.int32, (ROWS, HEAD), 1) < 64
        keys = jnp.where(low, lower, pltpu.roll(upper, 64, 1))
        values = jnp.where(low, pltpu.roll(lower, 64, 1), upper)
        kt[c, s] = keys.T.astype(bf16)
        v1[c, s, :, :HEAD] = values.astype(bf16)
        v1[c, s, :, HEAD:] = jnp.ones((ROWS, HEAD), bf16)

    def attend(qc, kc, h, first, last):
        query = q[qc, h]
        q_block = order[2 * cp + qc]
        best = None
        for s in range(N_CP):
            k_block = order[2 * s + kc]
            which = jnp.where(k_block < q_block, 0, jnp.where(k_block == q_block, 1, 2))
            scores = jnp.dot(query, kt[kc, s], preferred_element_type=f32) + bias[which]
            scr[:, s * ROWS : (s + 1) * ROWS] = scores
            here = jnp.maximum(scores[:, :HEAD], scores[:, HEAD:])
            best = here if best is None else jnp.maximum(best, here)
        new_top = jnp.broadcast_to(jnp.max(best, axis=1, keepdims=True), (ROWS, HEAD))
        if not first:
            old_top = top[qc, h]
            new_top = jnp.maximum(old_top, new_top)
        both = jnp.concatenate([new_top, new_top], axis=1)
        total = None
        for s in range(N_CP):
            weights = jnp.exp2(scr[:, s * ROWS : (s + 1) * ROWS] - both).astype(bf16)
            here = jnp.dot(weights, v1[kc, s], preferred_element_type=f32)
            total = here if total is None else total + here
        if not first:
            shrink = jnp.exp2(old_top - new_top)
            total = total + outs[qc, h] * jnp.concatenate([shrink, shrink], axis=1)
        if last:
            sums = total[:, HEAD:]
            columns = pl.ds(pl.multiple_of(h * HEAD, HEAD), HEAD)
            att[qc, :, columns] = (total[:, :HEAD] / sums).astype(bf16)
            normalizer = (new_top + jnp.log2(sums)) * LN2
            norm_out[pl.ds(h, 1), qc * ROWS : (qc + 1) * ROWS] = normalizer.T[:1]
        else:
            top[qc, h] = new_top
            outs[qc, h] = total

    def rs_copy(c, n, src, dst, device):
        return pltpu.make_async_remote_copy(
            src_ref=src,
            dst_ref=dst,
            send_sem=rs.at[c * 17 + n],
            recv_sem=rr.at[c * 17 + n],
            device_id=device,
            device_id_type=MESH,
        )

    def out_products(c):
        def one(i, unused):
            dp = 1 - i // 4
            dr = pick(i % 4, (2, 1, 3, 0))
            for dk, slot in ((1, i), (0, 8 + i)):
                columns = pl.ds(pl.multiple_of(tpi(dr, dp, dk) * FEAT, FEAT), FEAT)
                xg[c, slot] = jnp.dot(
                    att[c], wo[:, columns], preferred_element_type=f32
                ).astype(bf16)
                if dk == 1:
                    rs_copy(c, i, xg.at[c, i], ro.at[c, i], other).start()
            return unused

        lax.fori_loop(0, 8, one, 0)

    def both_cores(c, i):
        rs_copy(c, i, xg.at[c, i], ro.at[c, i], other).wait_recv()
        return xg[c, 8 + i].astype(f32) + ro[c, i].astype(f32)

    lo, hi = pl.ds(0, HALF), pl.ds(HALF, HALF)

    def far_out(c, p):
        i = 4 * p
        block = xg.at[c, 8 + i]
        block[...] = both_cores(c, i).astype(bf16)
        rs_copy(c, 8 + 4 * p, block.at[lo], ra.at[c, p], right).start()
        rs_copy(c, 9 + 4 * p, block.at[hi], rb.at[c, p], left).start()

    def near_out(c, p, side):
        i = 4 * p + 1 + side
        block = xg.at[c, 8 + i]
        term = both_cores(c, i)
        landed = (ra, rb)[side].at[c, p]
        rs_copy(c, 8 + side + 4 * p, landed, landed, left).wait_recv()
        moved = landed[...].astype(f32)
        if side == 0:
            block[:HALF] = (term[:HALF] + moved).astype(bf16)
            block[HALF:] = term[HALF:].astype(bf16)
        else:
            block[:HALF] = term[:HALF].astype(bf16)
            block[HALF:] = (term[HALF:] + moved).astype(bf16)
        rs_copy(
            c, 10 + side + 4 * p, block, (rc, rd)[side].at[c, p], (right, left)[side]
        ).start()

    def here_in(c, p):
        i = 4 * p + 3
        term = both_cores(c, i)
        for side in range(2):
            landed = (rc, rd)[side].at[c, p]
            rs_copy(c, 10 + side + 4 * p, landed, landed, left).wait_recv()
            term = term + landed[...].astype(f32)
        block = xg.at[c, 8 + i]
        if p == 0:
            block[...] = term.astype(bf16)
            rs_copy(c, 16, block, ry.at[c], pair).start()
        else:
            rs_copy(c, 16, block, ry.at[c], pair).wait_recv()
            proj[c * ROWS : (c + 1) * ROWS] = (term + ry[c].astype(f32)).astype(bf16)

    def rs_drain(c):
        whole, half = xg.at[c, 0], xg.at[c, 0, lo]
        for n in range(17):
            ref = half if n in (8, 9, 12, 13) else whole
            rs_copy(c, n, ref, ref, other).wait_send()

    def when(i, n, action):
        pl.when(i == n)(action)

    def gather_step(c, i):
        block_of = (None, 0, None, None, 1, 2, None, 3, None, 4, None, None, 5, 6, None, 7)
        if c == 0:
            for copy in w_copies(i):
                copy.wait()

        def events(n):
            if n == 2:
                g.from_left(c, 0) if c == 0 else None
            if n == 3:
                g.from_right(c, 0) if c == 0 else None
            if n == 6:
                if c == 0:
                    g.from_pair(0)
                    g.from_left(1, 0)
                    g.from_right(1, 0)
                g.from_far(c, 0)
            if n == 8 and c == 1:
                g.from_pair(1)
            if n == 10:
                g.from_left(c, 1)
            if n == 11:
                g.from_right(c, 1)
            if n == 14:
                g.from_far(c, 1)
            if block_of[n] is not None:
                g.from_core(c, block_of[n])
            if c == 1:
                if n == 1:
                    kv.from_left(0, 0)
                    kv.from_right(0, 0)
                if n == 3:
                    kv.from_pair(0)
                if n == 5:
                    kv.from_far(0, 0)
                    kv.from_left(0, 1)
                    kv.from_right(0, 1)
                if n == 7:
                    kv.from_far(0, 1)

        for n in range(1, 16):
            when(i, n, functools.partial(events, n))
        project(c, i)

    def steps(c):
        def one(i, unused):
            gather_step(c, i)
            return unused

        lax.fori_loop(0, 16, one, 0)

    def each(count, body):
        def one(i, unused):
            body(i)
            return unused

        lax.fori_loop(0, count, one, 0)

    def kv_landed(c):
        for b in range(8):
            kv.from_core(c, b)
        each(N_CP, functools.partial(assemble, c))

    steps(0)
    finish(0)
    steps(1)
    finish(1)
    kv_landed(0)
    g.drain(0)
    g.drain(1)

    each(4, lambda h: attend(0, 0, h, True, False))
    kv.from_left(1, 0)
    kv.from_right(1, 0)
    kv.from_pair(1)
    each(4, lambda h: attend(1, 0, h, True, False))
    kv.from_far(1, 0)
    kv.from_left(1, 1)
    kv.from_right(1, 1)
    kv.from_far(1, 1)
    kv_landed(1)
    each(4, lambda h: attend(0, 1, h, False, True))
    wo_copy.wait()
    out_products(0)
    far_out(0, 0)
    far_out(0, 1)

    def last_unit(h):
        attend(1, 1, h, False, True)

        def send(p):
            near_out(0, p, 0)
            near_out(0, p, 1)

        when(h, 1, lambda: send(0))
        when(h, 3, lambda: send(1))

    each(4, last_unit)
    out_products(1)
    far_out(1, 0)
    far_out(1, 1)
    here_in(0, 0)
    for p in range(2):
        near_out(1, p, 0)
        near_out(1, p, 1)
    here_in(0, 1)
    here_in(1, 0)
    here_in(1, 1)
    for c in range(2):
        kv.drain(c)
        rs_drain(c)


def shards(
    checkpoint, norm_gain, query_weight, key_weight, value_weight, output_weight, block_order
):
    context_rank, tensor_rank = lax.axis_index("cp"), lax.axis_index("tp")
    own_blocks = lax.dynamic_slice_in_dim(block_order, 2 * context_rank, 2)
    offsets = jnp.arange(ROWS, dtype=jnp.int32)
    positions = (own_blocks[:, None] * ROWS + offsets[None, :]).reshape(2 * ROWS).astype(f32)
    lane = jnp.arange(HEAD, dtype=jnp.int32)
    sign = jnp.where(lane % 2 == 0, -1.0, 1.0).astype(f32)
    scale = math.log2(math.e) / math.sqrt(HEAD)

    def table(first_pair):
        pairs = (first_pair + lane // 2).astype(f32)
        angles = positions[:, None] * (rope_base ** (-2.0 * pairs / HEAD))[None, :]
        return jnp.cos(angles), jnp.sin(angles) * sign

    cosine, sine = table(0)
    k_cosine, k_sine = table((tensor_rank % 2) * 32)
    is_key = (lane < 64)[None, :]
    k_cosine, k_sine = jnp.where(is_key, k_cosine, 1.0), jnp.where(is_key, k_sine, 0.0)
    kv_weight = jnp.concatenate([key_weight, value_weight], axis=1)

    vmem = pl.BlockSpec(memory_space=pltpu.VMEM)
    hbm = pl.BlockSpec(memory_space=pl.ANY)
    dma = pltpu.SemaphoreType.DMA
    return pl.pallas_call(
        kernel,
        out_shape=(
            jax.ShapeDtypeStruct((2 * ROWS, FEAT), bf16),
            jax.ShapeDtypeStruct((4, 2 * ROWS), f32),
        ),
        in_specs=[pl.BlockSpec(memory_space=pltpu.SMEM), hbm, vmem, vmem, vmem, vmem, vmem, hbm, hbm, hbm],
        out_specs=(vmem, vmem),
        scratch_shapes=[
            pltpu.VMEM((2, N_TP, ROWS, FEAT), bf16),
            pltpu.VMEM((D, FEAT), bf16),
            pltpu.VMEM((D, HEAD), bf16),
            pltpu.VMEM((FEAT, D), bf16),
            pltpu.VMEM((2, ROWS, FEAT + HEAD), f32),
            pltpu.VMEM((2, ROWS, HEAD), f32),
            pltpu.VMEM((2, 4, ROWS, HEAD), bf16),
            pltpu.VMEM((2, 2, N_CP, ROWS, HEAD), bf16),
            pltpu.VMEM((2, N_CP, HEAD, ROWS), bf16),
            pltpu.VMEM((2, N_CP, ROWS, 2 * HEAD), bf16),
            pltpu.VMEM((ROWS, N_CP * ROWS), f32),
            pltpu.VMEM((2, 4, ROWS, HEAD), f32),
            pltpu.VMEM((2, 4, ROWS, 2 * HEAD), f32),
            pltpu.VMEM((2, ROWS, FEAT), bf16),
            pltpu.VMEM((3, ROWS, ROWS), f32),
            pltpu.VMEM((2, 8, ROWS, FEAT), bf16),
            pltpu.VMEM((2, 2, HALF, FEAT), bf16),
            pltpu.VMEM((2, 2, HALF, FEAT), bf16),
            pltpu.VMEM((2, 2, ROWS, FEAT), bf16),
            pltpu.VMEM((2, 2, ROWS, FEAT), bf16),
            pltpu.VMEM((2, ROWS, FEAT), bf16),
            dma((2,)),
            dma((32,)),
            dma,
            dma((34,)),
            dma((34,)),
            dma((34,)),
            dma((34,)),
            dma((34,)),
            dma((34,)),
        ],
        compiler_params=pltpu.CompilerParams(
            collective_id=0, has_side_effects=True, vmem_limit_bytes=67000000
        ),
        name="sublayer",
    )(
        block_order,
        checkpoint,
        norm_gain.reshape(N_TP, FEAT),
        cosine * scale,
        sine * scale,
        k_cosine,
        k_sine,
        query_weight,
        kv_weight,
        output_weight,
    )


def solution(mesh):
    return jax.shard_map(
        shards,
        mesh=mesh,
        in_specs=(
            P("cp", "tp"),
            P(),
            P(None, "tp"),
            P(None, "tp"),
            P(None, "tp"),
            P("tp", None),
            P(),
        ),
        out_specs=(P("cp", "tp"), P("tp", "cp")),
        check_vma=False,
    )
```

```python
import functools
import math

import jax
import jax.numpy as jnp
from jax import lax
from jax.experimental import pallas as pl
from jax.experimental.pallas import tpu as pltpu
from jax.sharding import PartitionSpec as P

MESH = pl.DeviceIdType.MESH
HEAD = 128
ROWS = 256
FEAT = 512
HALF = ROWS // 2
N_TP = 16
N_CP = 8
D = 8192
rope_base = 500000.0
norm_epsilon = 1e-05
masked_score = -1e30
LN2 = math.log(2.0)

f32 = jnp.float32
bf16 = jnp.bfloat16


def pick(i, values):
    out = values[-1]
    for n in range(len(values) - 2, -1, -1):
        out = jnp.where(i == n, values[n], out)
    return out


class Gather:
    def __init__(self, slot, ssem, rsem, right, left, pair, core):
        self.slot, self.ssem, self.rsem = slot, ssem, rsem
        self.right, self.left, self.pair, self.core = right, left, pair, core

    def ref(self, c, b, dk=0, rows=None):
        ref = self.slot(c, b, dk)
        return ref if rows is None else ref.at[pl.ds(rows * HALF, HALF)]

    def copy(self, c, n, ref, device):
        return pltpu.make_async_remote_copy(
            src_ref=ref,
            dst_ref=ref,
            send_sem=self.ssem.at[c * 16 + n],
            recv_sem=self.rsem.at[c * 16 + n],
            device_id=device,
            device_id_type=MESH,
        )

    def send_core(self, c, b):
        self.copy(c, 8 + b, self.ref(c, b), self.core).start()

    def start(self, c):
        own = self.ref(c, 0)
        self.copy(c, 6, own, self.pair).start()
        self.copy(c, 0, own, self.right).start()
        self.copy(c, 3, own, self.left).start()
        self.send_core(c, 0)

    def from_left(self, c):
        self.copy(c, 0, self.ref(c, 1), self.left).wait_recv()
        self.copy(c, 1, self.ref(c, 1, rows=0), self.right).start()
        self.send_core(c, 1)

    def from_right(self, c):
        self.copy(c, 3, self.ref(c, 2), self.right).wait_recv()
        self.copy(c, 4, self.ref(c, 2, rows=1), self.left).start()
        self.send_core(c, 2)

    def from_pair(self, c):
        block = self.ref(c, 4)
        self.copy(c, 6, block, self.pair).wait_recv()
        self.copy(c, 2, block, self.right).start()
        self.copy(c, 5, block, self.left).start()
        self.send_core(c, 4)

    def from_far(self, c):
        self.copy(c, 1, self.ref(c, 3, rows=0), self.left).wait_recv()
        self.copy(c, 4, self.ref(c, 3, rows=1), self.right).wait_recv()
        self.copy(c, 7, self.ref(c, 3), self.pair).start()
        self.send_core(c, 3)

    def from_sides(self, c):
        self.copy(c, 2, self.ref(c, 5), self.left).wait_recv()
        self.send_core(c, 5)
        self.copy(c, 5, self.ref(c, 6), self.right).wait_recv()
        self.send_core(c, 6)

    def from_last(self, c):
        self.copy(c, 7, self.ref(c, 7), self.pair).wait_recv()
        self.send_core(c, 7)

    def from_core(self, c, b):
        self.copy(c, 8 + b, self.ref(c, b, dk=1), self.core).wait_recv()

    def drain(self, c):
        for n in range(16):
            ref = self.ref(c, 0, rows=0 if n in (1, 4) else None)
            self.copy(c, n, ref, self.core).wait_send()


def kernel(
    order, x_hbm, gain, wq_hbm, wk_hbm, wv_hbm, wo_hbm,
    proj, norm_out,
    xg, wq, wkv, wo, acc, ss, cos_t, sin_t, q, kvg, kt, v1, scr_a, scr_b, top, outs, att, bias,
    ro, ra, rb, rc, rd, re, ry,
    x_sem, w_sem, wo_sem, gs, gr, ks, kr, rs, rr,
):
    tp, cp = lax.axis_index("tp"), lax.axis_index("cp")
    core, yh, xx = tp % 2, (tp // 2) % 2, tp // 4
    yl, zz = cp % 2, cp // 2

    def tpi(dr, dp, dk):
        return (((xx + dr) % 4) * 2 + (yh + dp) % 2) * 2 + (core + dk) % 2

    def cpi(dr, dp):
        return ((zz + dr) % 4) * 2 + (yl + dp) % 2

    right, left = {"tp": tpi(1, 0, 0)}, {"tp": tpi(3, 0, 0)}
    pair, other = {"tp": tpi(0, 1, 0)}, {"tp": tpi(0, 0, 1)}
    up, down, beside = {"cp": cpi(1, 0)}, {"cp": cpi(3, 0)}, {"cp": cpi(0, 1)}

    ring_of = (0, 3, 1, 2)

    def tp_slot(b, dk):
        dr = ring_of[b % 4] if isinstance(b, int) else pick(b % 4, ring_of)
        return tpi(dr, b // 4, dk)

    x_copies = [
        pltpu.make_async_copy(x_hbm.at[pl.ds(c * ROWS, ROWS)], xg.at[c, tp], x_sem.at[c])
        for c in range(2)
    ]
    for copy in x_copies:
        copy.start()

    def wq_copy(b, dk):
        rows = pl.ds(pl.multiple_of(tp_slot(b, dk) * FEAT, FEAT), FEAT)
        return pltpu.make_async_copy(wq_hbm.at[rows], wq.at[rows], w_sem.at[b * 2 + dk])

    wk_copy = pltpu.make_async_copy(wk_hbm, wkv.at[pl.ds(0, 64)], w_sem.at[16])
    wv_copy = pltpu.make_async_copy(wv_hbm, wkv.at[pl.ds(64, 64)], w_sem.at[17])
    wo_copy = pltpu.make_async_copy(wo_hbm, wo, wo_sem)

    barrier = pltpu.get_barrier_semaphore()
    neighbours = (right, left, pair, other, up, down, beside)
    for device in neighbours:
        pl.semaphore_signal(barrier, inc=1, device_id=device, device_id_type=MESH)

    wk_copy.start()
    wv_copy.start()
    for b in (0, 1, 2, 4, 3, 5, 6, 7):
        for dk in range(2):
            wq_copy(b, dk).start()
    wo_copy.start()

    pl.semaphore_wait(barrier, len(neighbours))

    g = Gather(lambda c, b, dk: xg.at[c, tp_slot(b, dk)], gs, gr, right, left, pair, other)
    kv = Gather(
        lambda c, b, dk: kvg.at[c, (core + dk) % 2, cpi(ring_of[b % 4], b // 4)],
        ks, kr, up, down, beside, other,
    )

    for c in range(2):
        x_copies[c].wait()
        g.start(c)

    row_id = lax.broadcasted_iota(jnp.int32, (ROWS, ROWS), 0)
    col_id = lax.broadcasted_iota(jnp.int32, (ROWS, ROWS), 1)
    bias[0] = jnp.zeros((ROWS, ROWS), f32)
    bias[1] = jnp.where(col_id <= row_id, 0.0, masked_score).astype(f32)
    bias[2] = jnp.full((ROWS, ROWS), masked_score, f32)
    acc[...] = jnp.zeros_like(acc)
    ss[...] = jnp.zeros_like(ss)

    even = (lax.broadcasted_iota(jnp.int32, (ROWS, HEAD), 1) % 2) == 0
    low = lax.broadcasted_iota(jnp.int32, (ROWS, HEAD), 1) < 64

    def make_tables():
        lane8 = lax.broadcasted_iota(jnp.int32, (8, HEAD), 1)
        rate8 = jnp.exp2((lane8 // 2).astype(f32) * (-2.0 / HEAD * math.log2(rope_base)))
        rate = jnp.broadcast_to(rate8[:1], (ROWS, HEAD))
        angle = lax.broadcasted_iota(jnp.int32, (ROWS, HEAD), 0).astype(f32) * rate
        cos_r, sin_r = jnp.cos(angle), jnp.sin(angle)
        sign = jnp.where(even, -1.0, 1.0).astype(f32)
        for c in range(2):
            start = (order[2 * cp + c] * ROWS).astype(f32) * rate8
            cos_b, sin_b = jnp.cos(start)[:1], jnp.sin(start)[:1]
            cos_t[c] = cos_b * cos_r - sin_b * sin_r
            sin_t[c] = (sin_b * cos_r + cos_b * sin_r) * sign

    make_tables()

    def project(c, b, dk):
        j = tp_slot(b, dk)
        wide = xg[c, j].astype(f32)
        square = wide * wide
        ss[c] += square[:, :128] + square[:, 128:256] + square[:, 256:384] + square[:, 384:]
        scaled = jnp.concatenate(
            [
                (wide[:, n * HEAD : (n + 1) * HEAD] * gain[pl.ds(4 * j + n, 1), :]).astype(bf16)
                for n in range(4)
            ],
            axis=1,
        )
        rows = pl.ds(pl.multiple_of(j * FEAT, FEAT), FEAT)
        acc[c, :, :FEAT] += jnp.dot(scaled, wq[rows, :], preferred_element_type=f32)
        acc[c, :, FEAT:] += lax.dot_general(
            scaled, wkv[:, rows], (((1,), (1,)), ((), ())), preferred_element_type=f32
        )

    def turn(y, cosine, sine):
        swapped = jnp.where(even, pltpu.roll(y, HEAD - 1, 1), pltpu.roll(y, 1, 1))
        return y * cosine + swapped * sine

    def finish(c):
        scale = lax.rsqrt(jnp.sum(ss[c], axis=1, keepdims=True) * (1.0 / D) + norm_epsilon)
        scale = jnp.broadcast_to(scale, (ROWS, HEAD))
        cosine, sine = cos_t[c], sin_t[c]
        k_cos = jnp.where(core == 0, cosine, pltpu.roll(cosine, 64, 1))
        k_sin = jnp.where(core == 0, sine, pltpu.roll(sine, 64, 1))
        k_cos, k_sin = jnp.where(low, k_cos, 1.0), jnp.where(low, k_sin, 0.0)
        kvg[c, core, cp] = turn(acc[c, :, FEAT:] * scale, k_cos, k_sin).astype(bf16)
        kv.start(c)
        q_scale = scale * (math.log2(math.e) / math.sqrt(HEAD))
        for h in range(4):
            y = acc[c, :, h * HEAD : (h + 1) * HEAD] * q_scale
            q[c, h] = turn(y, cosine, sine).astype(bf16)

    def assemble(c, s):
        lower, upper = kvg[c, 0, s].astype(f32), kvg[c, 1, s].astype(f32)
        keys = jnp.where(low, lower, pltpu.roll(upper, 64, 1))
        values = jnp.where(low, pltpu.roll(lower, 64, 1), upper)
        kt[c, s] = keys.T.astype(bf16)
        rows = pl.ds(pl.multiple_of(s * ROWS, ROWS), ROWS)
        v1[c, rows, :HEAD] = values.astype(bf16)
        v1[c, rows, HEAD:] = jnp.ones((ROWS, HEAD), bf16)

    def unit(qc, kc, first, last, between=()):
        q_block = order[2 * cp + qc]
        which = []
        for s in range(N_CP):
            k_block = order[2 * s + kc]
            which.append(jnp.where(k_block < q_block, 0, jnp.where(k_block == q_block, 1, 2)))
        group = 4
        tops = {}

        def score(h, s, best):
            scr = (scr_a, scr_b)[h % 2]
            scores = jnp.dot(q[qc, h], kt[kc, s], preferred_element_type=f32) + bias[which[s]]
            scr[:, s * ROWS : (s + 1) * ROWS] = scores
            here = jnp.maximum(scores[:, :HEAD], scores[:, HEAD:])
            return here if best is None else jnp.maximum(best, here)

        def settle(h, best):
            new_top = jnp.broadcast_to(jnp.max(best, axis=1, keepdims=True), (ROWS, HEAD))
            tops[h] = new_top if first else jnp.maximum(top[qc, h], new_top)

        def weigh(h, s, total):
            scr = (scr_a, scr_b)[h % 2]
            both = jnp.concatenate([tops[h]] * 2, axis=1)
            weights = [
                jnp.exp2(scr[:, n * ROWS : (n + 1) * ROWS] - both).astype(bf16)
                for n in range(s, s + group)
            ]
            here = jnp.dot(
                jnp.concatenate(weights, axis=1),
                v1[kc, s * ROWS : (s + group) * ROWS],
                preferred_element_type=f32,
            )
            return here if total is None else total + here

        def close(h, total):
            if not first:
                shrink = jnp.exp2(top[qc, h] - tops[h])
                total = total + outs[qc, h] * jnp.concatenate([shrink, shrink], axis=1)
            if last:
                sums = total[:, HEAD:]
                att[qc, :, h * HEAD : (h + 1) * HEAD] = (total[:, :HEAD] / sums).astype(bf16)
                normalizer = (tops[h] + jnp.log2(sums)) * LN2
                norm_out[h : h + 1, qc * ROWS : (qc + 1) * ROWS] = normalizer.T[:1]
            else:
                top[qc, h] = tops[h]
                outs[qc, h] = total

        best = None
        for s in range(N_CP):
            best = score(0, s, best)
        settle(0, best)
        for h in range(4):
            best = total = None
            for s in range(N_CP):
                if h < 3:
                    best = score(h + 1, s, best)
                if s % group == group - 1:
                    total = weigh(h, s - group + 1, total)
            close(h, total)
            if h < 3:
                settle(h + 1, best)
            if h < len(between) and between[h] is not None:
                between[h]()

    def rs_copy(c, n, src, dst, device):
        return pltpu.make_async_remote_copy(
            src_ref=src,
            dst_ref=dst,
            send_sem=rs.at[c * 16 + n],
            recv_sem=rr.at[c * 16 + n],
            device_id=device,
            device_id_type=MESH,
        )

    lo, hi = pl.ds(0, HALF), pl.ds(HALF, HALF)
    dests = ((2, 1), (2, 0), (1, 1), (3, 1), (1, 0), (3, 0), (0, 1), (0, 0))

    def both_cores(c, i):
        rs_copy(c, i, xg.at[c, i], ro.at[c, i], other).wait_recv()
        return xg[c, 8 + i].astype(f32) + ro[c, i].astype(f32)

    def far_pair(c):
        block = xg.at[c, 8]
        block[...] = both_cores(c, 0).astype(bf16)
        rs_copy(c, 8, block, re.at[c], pair).start()

    def far_out(c):
        block = xg.at[c, 9]
        term = both_cores(c, 1)
        rs_copy(c, 8, re.at[c], re.at[c], pair).wait_recv()
        block[...] = (term + re[c].astype(f32)).astype(bf16)
        rs_copy(c, 9, block.at[lo], ra.at[c], right).start()
        rs_copy(c, 10, block.at[hi], rb.at[c], left).start()

    def near_pair(c, side):
        block = xg.at[c, 10 + side]
        block[...] = both_cores(c, 2 + side).astype(bf16)
        rs_copy(c, 11 + side, block, (rc, rd)[side].at[c, 1], (right, left)[side]).start()

    def near_out(c, side):
        block = xg.at[c, 12 + side]
        term = both_cores(c, 4 + side)
        landed = (ra, rb)[side].at[c]
        rs_copy(c, 9 + side, landed, landed, left).wait_recv()
        moved = landed[...].astype(f32)
        if side == 0:
            block[:HALF] = (term[:HALF] + moved).astype(bf16)
            block[HALF:] = term[HALF:].astype(bf16)
        else:
            block[:HALF] = term[:HALF].astype(bf16)
            block[HALF:] = (term[HALF:] + moved).astype(bf16)
        rs_copy(c, 13 + side, block, (rc, rd)[side].at[c, 0], (right, left)[side]).start()

    def here_in(c, p):
        term = both_cores(c, 7 - p)
        for side in range(2):
            landed = (rc, rd)[side].at[c, p]
            rs_copy(c, (13, 11)[p] + side, landed, landed, left).wait_recv()
            term = term + landed[...].astype(f32)
        block = xg.at[c, 14]
        if p == 1:
            block[...] = term.astype(bf16)
            rs_copy(c, 15, block, ry.at[c], pair).start()
        else:
            rs_copy(c, 15, block, ry.at[c], pair).wait_recv()
            proj[c * ROWS : (c + 1) * ROWS] = (term + ry[c].astype(f32)).astype(bf16)

    def rs_drain(c):
        whole, half = xg.at[c, 0], xg.at[c, 0, lo]
        for n in range(16):
            ref = half if n in (9, 10) else whole
            rs_copy(c, n, ref, ref, other).wait_send()

    def when(i, n, action):
        pl.when(i == n)(action)

    def out_products(c, events):
        def one(i, unused):
            dr, dp = pick(i, [d[0] for d in dests]), pick(i, [d[1] for d in dests])
            for dk, slot in ((1, i), (0, 8 + i)):
                columns = pl.ds(pl.multiple_of(tpi(dr, dp, dk) * FEAT, FEAT), FEAT)
                xg[c, slot] = jnp.dot(
                    att[c], wo[:, columns], preferred_element_type=f32
                ).astype(bf16)
                if dk == 1:
                    rs_copy(c, i, xg.at[c, i], ro.at[c, i], other).start()
            for n, action in events.items():
                when(i, n, action)
            return unused

        lax.fori_loop(0, 8, one, 0)

    plan = (
        [(c, 0, dk) for dk in range(2) for c in range(2)]
        + [(0, 1, 0), (0, 2, 0), (0, 1, 1), (0, 2, 1)]
        + [(1, 1, 0), (1, 2, 0), (1, 1, 1), (1, 2, 1)]
        + [(0, 4, 0), (0, 4, 1), (1, 4, 0), (1, 4, 1)]
        + [(0, 3, 0), (0, 3, 1), (1, 3, 0), (1, 3, 1)]
        + [(0, 5, 0), (0, 6, 0), (0, 5, 1), (0, 6, 1)]
        + [(0, 7, 0), (0, 7, 1), (1, 7, 0), (1, 7, 1)]
        + [(1, 5, 0), (1, 6, 0), (1, 5, 1), (1, 6, 1)]
    )

    def gather_event(n):
        if n == 4:
            g.from_left(0)
            g.from_right(0)
        if n == 8:
            g.from_left(1)
            g.from_right(1)
            g.from_pair(0)
            g.from_pair(1)
        if n in (16, 18):
            g.from_far((n - 16) // 2)
        if n == 20:
            g.from_sides(0)
        if n == 24:
            g.from_last(0)
        if n == 26:
            g.from_last(1)
        if n == 28:
            kv.from_left(0)
            kv.from_right(0)
            kv.from_pair(0)
            g.from_sides(1)
        c, b, dk = plan[n]
        if dk:
            g.from_core(c, b)

    def steps(first, last):
        def one(i, unused):
            for n in range(first, last):
                if n in (4, 8, 16, 18, 20, 24, 26, 28) or plan[n][2]:
                    when(i, n, functools.partial(gather_event, n))
            code = pick(i - first, [(c * 8 + b) * 2 + dk for c, b, dk in plan[first:last]])
            c, b, dk = code // 16, (code // 2) % 8, code % 2
            pl.when(c == 0)(lambda: wq_copy(b, dk).wait())
            project(c, b, dk)
            return unused

        lax.fori_loop(first, last, one, 0)

    def each(count, body):
        def one(i, unused):
            body(i)
            return unused

        lax.fori_loop(0, count, one, 0)

    def kv_landed(c):
        for b in range(8):
            kv.from_core(c, b)
        each(N_CP, functools.partial(assemble, c))

    wk_copy.wait()
    wv_copy.wait()
    steps(0, 26)
    finish(0)
    steps(26, 32)
    finish(1)
    kv.from_far(0)
    kv.from_sides(0)
    kv.from_last(0)
    kv_landed(0)
    g.drain(0)
    g.drain(1)

    def sides1():
        kv.from_left(1)
        kv.from_right(1)
        kv.from_pair(1)

    def rest1():
        kv.from_far(1)
        kv.from_sides(1)

    unit(0, 0, True, False, (None, sides1, None, lambda: kv.from_far(1)))
    unit(1, 0, True, False, (lambda: kv.from_sides(1), lambda: kv.from_last(1)))
    kv_landed(1)
    unit(0, 1, False, True)
    wo_copy.wait()

    def first_sends(c):
        return {
            1: lambda: far_pair(c),
            3: lambda: near_pair(c, 0),
            4: lambda: near_pair(c, 1),
        }

    out_products(0, first_sends(0))
    unit(1, 1, False, True, (None, None, lambda: far_out(0), None))
    out_products(1, first_sends(1))
    here_in(0, 1)
    near_out(0, 0)
    near_out(0, 1)
    far_out(1)
    here_in(1, 1)
    near_out(1, 0)
    near_out(1, 1)
    here_in(0, 0)
    here_in(1, 0)
    for c in range(2):
        kv.drain(c)
        rs_drain(c)

def shards(
    checkpoint, norm_gain, query_weight, key_weight, value_weight, output_weight, block_order
):
    vmem = pl.BlockSpec(memory_space=pltpu.VMEM)
    hbm = pl.BlockSpec(memory_space=pl.ANY)
    dma = pltpu.SemaphoreType.DMA
    return pl.pallas_call(
        kernel,
        out_shape=(
            jax.ShapeDtypeStruct((2 * ROWS, FEAT), bf16),
            jax.ShapeDtypeStruct((4, 2 * ROWS), f32),
        ),
        in_specs=[pl.BlockSpec(memory_space=pltpu.SMEM), hbm, vmem, hbm, hbm, hbm, hbm],
        out_specs=(vmem, vmem),
        scratch_shapes=[
            pltpu.VMEM((2, N_TP, ROWS, FEAT), bf16),
            pltpu.VMEM((D, FEAT), bf16),
            pltpu.VMEM((HEAD, D), bf16),
            pltpu.VMEM((FEAT, D), bf16),
            pltpu.VMEM((2, ROWS, FEAT + HEAD), f32),
            pltpu.VMEM((2, ROWS, HEAD), f32),
            pltpu.VMEM((2, ROWS, HEAD), f32),
            pltpu.VMEM((2, ROWS, HEAD), f32),
            pltpu.VMEM((2, 4, ROWS, HEAD), bf16),
            pltpu.VMEM((2, 2, N_CP, ROWS, HEAD), bf16),
            pltpu.VMEM((2, N_CP, HEAD, ROWS), bf16),
            pltpu.VMEM((2, N_CP * ROWS, 2 * HEAD), bf16),
            pltpu.VMEM((ROWS, N_CP * ROWS), f32),
            pltpu.VMEM((ROWS, N_CP * ROWS), f32),
            pltpu.VMEM((2, 4, ROWS, HEAD), f32),
            pltpu.VMEM((2, 4, ROWS, 2 * HEAD), f32),
            pltpu.VMEM((2, ROWS, FEAT), bf16),
            pltpu.VMEM((3, ROWS, ROWS), f32),
            pltpu.VMEM((2, 8, ROWS, FEAT), bf16),
            pltpu.VMEM((2, HALF, FEAT), bf16),
            pltpu.VMEM((2, HALF, FEAT), bf16),
            pltpu.VMEM((2, 2, ROWS, FEAT), bf16),
            pltpu.VMEM((2, 2, ROWS, FEAT), bf16),
            pltpu.VMEM((2, ROWS, FEAT), bf16),
            pltpu.VMEM((2, ROWS, FEAT), bf16),
            dma((2,)),
            dma((18,)),
            dma,
            dma((32,)),
            dma((32,)),
            dma((32,)),
            dma((32,)),
            dma((32,)),
            dma((32,)),
        ],
        compiler_params=pltpu.CompilerParams(
            collective_id=0, has_side_effects=True, vmem_limit_bytes=67000000
        ),
        name="sublayer",
    )(
        block_order,
        checkpoint,
        norm_gain.reshape(D // HEAD, HEAD),
        query_weight,
        key_weight.T,
        value_weight.T,
        output_weight,
    )


def solution(mesh):
    return jax.shard_map(
        shards,
        mesh=mesh,
        in_specs=(
            P("cp", "tp"),
            P(),
            P(None, "tp"),
            P(None, "tp"),
            P(None, "tp"),
            P("tp", None),
            P(),
        ),
        out_specs=(P("cp", "tp"), P("tp", "cp")),
        check_vma=False,
    )
```

```python
import functools
import math

import jax
import jax.numpy as jnp
from jax import lax
from jax.experimental import pallas as pl
from jax.experimental.pallas import tpu as pltpu
from jax.sharding import PartitionSpec as P

MESH = pl.DeviceIdType.MESH
HEAD = 128
ROWS = 256
FEAT = 512
HALF = ROWS // 2
N_TP = 16
N_CP = 8
D = 8192
rope_base = 500000.0
norm_epsilon = 1e-05
masked_score = -1e30
LN2 = math.log(2.0)

f32 = jnp.float32
bf16 = jnp.bfloat16


def pick(i, values):
    out = values[-1]
    for n in range(len(values) - 2, -1, -1):
        out = jnp.where(i == n, values[n], out)
    return out


class Gather:
    def __init__(self, slot, ssem, rsem, right, left, pair, core=None):
        self.slot, self.ssem, self.rsem = slot, ssem, rsem
        self.right, self.left, self.pair, self.core = right, left, pair, core
        self.count = 10 if core is None else 18

    def ref(self, c, b, dk=0, rows=None):
        ref = self.slot(c, b, dk)
        return ref if rows is None else ref.at[pl.ds(rows * HALF, HALF)]

    def copy(self, c, n, ref, device):
        return pltpu.make_async_remote_copy(
            src_ref=ref,
            dst_ref=ref,
            send_sem=self.ssem.at[c * self.count + n],
            recv_sem=self.rsem.at[c * self.count + n],
            device_id=device,
            device_id_type=MESH,
        )

    def send_core(self, c, b):
        if self.core is not None:
            self.copy(c, 10 + b, self.ref(c, b), self.core).start()

    def start_pair(self, c):
        self.copy(c, 8, self.ref(c, 0), self.pair).start()
        self.send_core(c, 0)

    def start_ring(self, c):
        lower, upper = self.ref(c, 0, rows=0), self.ref(c, 0, rows=1)
        self.copy(c, 0, lower, self.right).start()
        self.copy(c, 4, upper, self.left).start()
        self.copy(c, 1, upper, self.right).start()
        self.copy(c, 5, lower, self.left).start()

    def pass_on(self, c):
        block = self.ref(c, 1, rows=0)
        self.copy(c, 0, block, self.left).wait_recv()
        self.copy(c, 2, block, self.right).start()
        block = self.ref(c, 2, rows=1)
        self.copy(c, 4, block, self.right).wait_recv()
        self.copy(c, 6, block, self.left).start()

    def from_sides(self, c):
        self.copy(c, 1, self.ref(c, 1, rows=1), self.left).wait_recv()
        self.send_core(c, 1)
        self.copy(c, 5, self.ref(c, 2, rows=0), self.right).wait_recv()
        self.send_core(c, 2)

    def from_pair(self, c):
        self.copy(c, 8, self.ref(c, 4), self.pair).wait_recv()
        self.send_core(c, 4)

    def pass_pair(self, c):
        block = self.ref(c, 4)
        self.copy(c, 3, block, self.right).start()
        self.copy(c, 7, block, self.left).start()

    def from_far(self, c):
        self.copy(c, 2, self.ref(c, 3, rows=0), self.left).wait_recv()
        self.copy(c, 6, self.ref(c, 3, rows=1), self.right).wait_recv()
        self.copy(c, 9, self.ref(c, 3), self.pair).start()
        self.send_core(c, 3)

    def from_pair_sides(self, c):
        self.copy(c, 3, self.ref(c, 5), self.left).wait_recv()
        self.send_core(c, 5)
        self.copy(c, 7, self.ref(c, 6), self.right).wait_recv()
        self.send_core(c, 6)

    def from_last(self, c):
        self.copy(c, 9, self.ref(c, 7), self.pair).wait_recv()
        self.send_core(c, 7)

    def from_core(self, c, b):
        self.copy(c, 10 + b, self.ref(c, b, dk=1), self.core).wait_recv()

    def drain(self, c):
        for n in range(self.count):
            ref = self.ref(c, 0, rows=0 if n in (0, 1, 2, 4, 5, 6) else None)
            self.copy(c, n, ref, self.pair).wait_send()


RING = (0, 3, 1, 2)
KEY_ORDER = (0, 1, 2, 4, 3, 5, 6, 7)
DESTS = ((2, 1), (2, 0), (1, 1), (3, 1), (1, 0), (3, 0), (0, 1), (0, 0))
PLAN = (
    (0, 0), (1, 0), (0, 1), (0, 2), (0, 4), (0, 3), (1, 1), (1, 2),
    (1, 4), (1, 3), (0, 7), (0, 5), (0, 6), (1, 7), (1, 5), (1, 6),
)


def kernel(
    order, x_hbm, gain, wq_hbm, wk_hbm, wv_hbm, wo_hbm,
    proj, norm_out,
    xg, wq, wkv, wo, acc_q, acc_kv, ss, part, part_q, part_kv, cos_t, sin_t, q, kvg, kt, v1,
    scr_a, scr_b, top, outs, att, bias, terms, ra, rb, rc, rd, re, ry,
    x_sem, w_sem, xs, xr, gs, gr, ks, kr, ps, pr, rs, rr,
):
    tp, cp = lax.axis_index("tp"), lax.axis_index("cp")
    core, yh, xx = tp % 2, (tp // 2) % 2, tp // 4
    yl, zz = cp % 2, cp // 2

    def tpi(dr, dp, dk):
        return (((xx + dr) % 4) * 2 + (yh + dp) % 2) * 2 + (core + dk) % 2

    def cpi(dr, dp):
        return ((zz + dr) % 4) * 2 + (yl + dp) % 2

    right, left = {"tp": tpi(1, 0, 0)}, {"tp": tpi(3, 0, 0)}
    pair, other = {"tp": tpi(0, 1, 0)}, {"tp": tpi(0, 0, 1)}
    up, down, beside = {"cp": cpi(1, 0)}, {"cp": cpi(3, 0)}, {"cp": cpi(0, 1)}

    def chip(b):
        dr = RING[b % 4] if isinstance(b, int) else pick(b % 4, RING)
        return ((xx + dr) % 4) * 2 + (yh + b // 4) % 2

    def tp_slot(b, dk):
        return chip(b) * 2 + (core + dk) % 2

    def kv_slot(b):
        dr = RING[b % 4] if isinstance(b, int) else pick(b % 4, RING)
        return cpi(dr, b // 4)

    x_copies = [
        pltpu.make_async_copy(x_hbm.at[pl.ds(c * ROWS, ROWS)], xg.at[c, tp // 2], x_sem.at[c])
        for c in range(2)
    ]
    for copy in x_copies:
        copy.start()

    def features(b, dk):
        return pl.ds(pl.multiple_of(tp_slot(b, dk) * FEAT, FEAT), FEAT)

    def to_other(n, src, dst):
        return pltpu.make_async_remote_copy(
            src_ref=src,
            dst_ref=dst,
            send_sem=xs.at[n],
            recv_sem=xr.at[n],
            device_id=other,
            device_id_type=MESH,
        )

    def wq_copy(b):
        return pltpu.make_async_copy(wq_hbm.at[features(b, 0)], wq.at[0, b], w_sem.at[b])

    def wo_copy(b):
        return pltpu.make_async_copy(wo_hbm.at[:, features(b, 0)], wo.at[0, b], w_sem.at[8 + b])

    def wq_across(b):
        return to_other(b, wq_hbm.at[features(b, 1)], wq.at[1, b])

    def wo_across(b):
        return to_other(8 + b, wo_hbm.at[:, features(b, 1)], wo.at[1, b])

    wk_copy = pltpu.make_async_copy(wk_hbm, wkv.at[pl.ds(0, 64)], w_sem.at[16])
    wv_copy = pltpu.make_async_copy(wv_hbm, wkv.at[pl.ds(64, 64)], w_sem.at[17])
    wk_across = to_other(16, wk_hbm, wkv.at[pl.ds(128, 64)])
    wv_across = to_other(17, wv_hbm, wkv.at[pl.ds(192, 64)])

    barrier = pltpu.get_barrier_semaphore()
    neighbours = (right, left, pair, other, up, down, beside)
    for device in neighbours:
        pl.semaphore_signal(barrier, inc=1, device_id=device, device_id_type=MESH)

    first_use = (0, 1, 2, 4, 3, 7, 5, 6)
    wk_copy.start()
    wv_copy.start()
    for b in first_use:
        wq_copy(b).start()
    for b in range(8):
        wo_copy(b).start()

    pl.semaphore_wait(barrier, len(neighbours))

    g = Gather(lambda c, b, dk: xg.at[c, chip(b)], gs, gr, right, left, pair)
    kv = Gather(
        lambda c, b, dk: kvg.at[c, (core + dk) % 2, kv_slot(b)], ks, kr, up, down, beside, other
    )

    x_copies[0].wait()
    g.start_pair(0)
    g.start_ring(0)
    x_copies[1].wait()
    g.start_pair(1)
    wk_across.start()
    wv_across.start()
    for b in first_use:
        wq_across(b).start()
    for b in range(8):
        wo_across(b).start()

    row_id = lax.broadcasted_iota(jnp.int32, (ROWS, ROWS), 0)
    col_id = lax.broadcasted_iota(jnp.int32, (ROWS, ROWS), 1)
    bias[0] = jnp.zeros((ROWS, ROWS), f32)
    bias[1] = jnp.where(col_id <= row_id, 0.0, masked_score).astype(f32)
    bias[2] = jnp.full((ROWS, ROWS), masked_score, f32)
    acc_q[...] = jnp.zeros_like(acc_q)
    acc_kv[...] = jnp.zeros_like(acc_kv)
    ss[...] = jnp.zeros_like(ss)

    even = (lax.broadcasted_iota(jnp.int32, (ROWS, HEAD), 1) % 2) == 0
    low = lax.broadcasted_iota(jnp.int32, (ROWS, HEAD), 1) < 64

    def make_tables():
        lane8 = lax.broadcasted_iota(jnp.int32, (8, HEAD), 1)
        rate8 = jnp.exp2((lane8 // 2).astype(f32) * (-2.0 / HEAD * math.log2(rope_base)))
        rate = jnp.broadcast_to(rate8[:1], (ROWS, HEAD))
        angle = lax.broadcasted_iota(jnp.int32, (ROWS, HEAD), 0).astype(f32) * rate
        cos_r, sin_r = jnp.cos(angle), jnp.sin(angle)
        sign = jnp.where(even, -1.0, 1.0).astype(f32)
        for c in range(2):
            start = (order[2 * cp + c] * ROWS).astype(f32) * rate8
            cos_b, sin_b = jnp.cos(start)[:1], jnp.sin(start)[:1]
            cos_t[c] = cos_b * cos_r - sin_b * sin_r
            sin_t[c] = (sin_b * cos_r + cos_b * sin_r) * sign

    make_tables()

    def project(c, b):
        wide = xg[c, chip(b)].astype(f32)
        square = wide * wide
        ss[c] += square[:, :128] + square[:, 128:256] + square[:, 256:384] + square[:, 384:]
        j = tp_slot(b, 0)
        scaled = jnp.concatenate(
            [
                (wide[:, n * HEAD : (n + 1) * HEAD] * gain[pl.ds(4 * j + n, 1), :]).astype(bf16)
                for n in range(4)
            ],
            axis=1,
        )
        acc_kv[c] += lax.dot_general(
            scaled, wkv[:, features(b, 0)], (((1,), (1,)), ((), ())), preferred_element_type=f32
        )
        for owner in range(2):
            acc_q[c, owner] += jnp.dot(scaled, wq[owner, b], preferred_element_type=f32)

    def partial_copy(c, n):
        if n == 0:
            return to_other(18 + c, part.at[c], part_kv.at[c])
        return to_other(20 + c, acc_q.at[c, 1], part_q.at[c])

    def send_partials(c):
        part[c, :, :HEAD] = acc_kv[c, :, HEAD:]
        part[c, :, HEAD:] = ss[c]
        partial_copy(c, 0).start()
        partial_copy(c, 1).start()

    def turn(y, cosine, sine):
        swapped = jnp.where(even, pltpu.roll(y, HEAD - 1, 1), pltpu.roll(y, 1, 1))
        return y * cosine + swapped * sine

    def finish_kv(c):
        partial_copy(c, 0).wait_recv()
        squares = jnp.sum(ss[c] + part_kv[c, :, HEAD:], axis=1, keepdims=True)
        scale = jnp.broadcast_to(lax.rsqrt(squares * (1.0 / D) + norm_epsilon), (ROWS, HEAD))
        ss[c] = scale
        cosine, sine = cos_t[c], sin_t[c]
        k_cos = jnp.where(core == 0, cosine, pltpu.roll(cosine, 64, 1))
        k_sin = jnp.where(core == 0, sine, pltpu.roll(sine, 64, 1))
        k_cos, k_sin = jnp.where(low, k_cos, 1.0), jnp.where(low, k_sin, 0.0)
        both = (acc_kv[c, :, :HEAD] + part_kv[c, :, :HEAD]) * scale
        kvg[c, core, cp] = turn(both, k_cos, k_sin).astype(bf16)
        kv.start_pair(c)
        kv.start_ring(c)

    def finish_q(c):
        partial_copy(c, 1).wait_recv()
        cosine, sine = cos_t[c], sin_t[c]
        q_scale = ss[c] * (math.log2(math.e) / math.sqrt(HEAD))
        for h in range(4):
            lanes = slice(h * HEAD, (h + 1) * HEAD)
            y = (acc_q[c, 0, :, lanes] + part_q[c, :, lanes]) * q_scale
            q[c, h] = turn(y, cosine, sine).astype(bf16)

    def each(first, last, body):
        def one(i, unused):
            body(i)
            return unused

        lax.fori_loop(first, last, one, 0)

    def when(i, n, action):
        pl.when(i == n)(action)

    def assemble(c, p):
        slot = kv_slot(pick(p, KEY_ORDER))
        lower, upper = kvg[c, 0, slot].astype(f32), kvg[c, 1, slot].astype(f32)
        keys = jnp.where(low, lower, pltpu.roll(upper, 64, 1))
        values = jnp.where(low, pltpu.roll(lower, 64, 1), upper)
        kt[c, p] = keys.T.astype(bf16)
        rows = pl.ds(pl.multiple_of(p * ROWS, ROWS), ROWS)
        v1[c, rows, :HEAD] = values.astype(bf16)
        v1[c, rows, HEAD:] = jnp.ones((ROWS, HEAD), bf16)

    def landed(c, first, last):
        for b in KEY_ORDER[first:last]:
            kv.from_core(c, b)
        each(first, last, functools.partial(assemble, c))

    def unit(qc, kc, start, stop, first, last, between=()):
        q_block = order[2 * cp + qc]
        which = {}
        for p in range(start, stop):
            k_block = order[2 * kv_slot(KEY_ORDER[p]) + kc]
            which[p] = jnp.where(k_block < q_block, 0, jnp.where(k_block == q_block, 1, 2))
        group = 4
        tops = {}

        def score(h, p, best):
            scr = (scr_a, scr_b)[h % 2]
            scores = jnp.dot(q[qc, h], kt[kc, p], preferred_element_type=f32) + bias[which[p]]
            scr[:, p * ROWS : (p + 1) * ROWS] = scores
            here = jnp.maximum(scores[:, :HEAD], scores[:, HEAD:])
            return here if best is None else jnp.maximum(best, here)

        def settle(h, best):
            new_top = jnp.broadcast_to(jnp.max(best, axis=1, keepdims=True), (ROWS, HEAD))
            tops[h] = new_top if first else jnp.maximum(top[qc, h], new_top)

        def weigh(h, p, total):
            scr = (scr_a, scr_b)[h % 2]
            both = jnp.concatenate([tops[h]] * 2, axis=1)
            weights = [
                jnp.exp2(scr[:, n * ROWS : (n + 1) * ROWS] - both).astype(bf16)
                for n in range(p, p + group)
            ]
            here = jnp.dot(
                jnp.concatenate(weights, axis=1),
                v1[kc, p * ROWS : (p + group) * ROWS],
                preferred_element_type=f32,
            )
            return here if total is None else total + here

        def close(h, total):
            if not first:
                shrink = jnp.exp2(top[qc, h] - tops[h])
                total = total + outs[qc, h] * jnp.concatenate([shrink, shrink], axis=1)
            if last:
                sums = total[:, HEAD:]
                att[qc, 0, h] = (total[:, :HEAD] / sums).astype(bf16)
                att_copy(qc, h).start()
                normalizer = (tops[h] + jnp.log2(sums)) * LN2
                norm_out[h : h + 1, qc * ROWS : (qc + 1) * ROWS] = normalizer.T[:1]
            else:
                top[qc, h] = tops[h]
                outs[qc, h] = total

        best = None
        for p in range(start, stop):
            best = score(0, p, best)
        settle(0, best)
        for h in range(4):
            best = total = None
            for p in range(start, stop):
                if h < 3:
                    best = score(h + 1, p, best)
                if p % group == group - 1:
                    total = weigh(h, p - group + 1, total)
            close(h, total)
            if h < 3:
                settle(h + 1, best)
            if h < len(between) and between[h] is not None:
                between[h]()

    def att_copy(c, h):
        return pltpu.make_async_remote_copy(
            src_ref=att.at[c, 0, h],
            dst_ref=att.at[c, 1, h],
            send_sem=ps.at[c * 4 + h],
            recv_sem=pr.at[c * 4 + h],
            device_id=other,
            device_id_type=MESH,
        )

    def rs_copy(c, n, src, dst, device):
        return pltpu.make_async_remote_copy(
            src_ref=src,
            dst_ref=dst,
            send_sem=rs.at[c * 10 + n],
            recv_sem=rr.at[c * 10 + n],
            device_id=device,
            device_id_type=MESH,
        )

    lo, hi = pl.ds(0, HALF), pl.ds(HALF, HALF)
    ways = (right, left)

    def far_pair(c):
        rs_copy(c, 0, terms.at[c, 0], re.at[c], pair).start()

    def far_out(c):
        block = terms.at[c, 1]
        rs_copy(c, 0, re.at[c], re.at[c], pair).wait_recv()
        block[...] = (block[...].astype(f32) + re[c].astype(f32)).astype(bf16)
        rs_copy(c, 1, block.at[lo], ra.at[c], right).start()
        rs_copy(c, 2, block.at[hi], rb.at[c], left).start()

    def near_pair(c, side):
        rs_copy(c, 3 + side, terms.at[c, 2 + side], (rc, rd)[side].at[c, 1], ways[side]).start()

    def near_free(c, side):
        half = (hi, lo)[side]
        rs_copy(
            c, 5 + side, terms.at[c, 4 + side].at[half], (rc, rd)[side].at[c, 0].at[half], ways[side]
        ).start()

    def near_joined(c, side):
        half = (lo, hi)[side]
        block, moved = terms.at[c, 4 + side].at[half], (ra, rb)[side].at[c]
        rs_copy(c, 1 + side, moved, moved, left).wait_recv()
        block[...] = (block[...].astype(f32) + moved[...].astype(f32)).astype(bf16)
        rs_copy(c, 7 + side, block, (rc, rd)[side].at[c, 0].at[half], ways[side]).start()

    def here_in(c, p):
        term = terms[c, 7 - p].astype(f32)
        for side in range(2):
            block = (rc, rd)[side].at[c, p]
            if p == 1:
                rs_copy(c, 3 + side, block, block, left).wait_recv()
            else:
                for n, half in ((5, (hi, lo)[side]), (7, (lo, hi)[side])):
                    rs_copy(c, n + side, block.at[half], block.at[half], left).wait_recv()
            term = term + block[...].astype(f32)
        if p == 1:
            block = terms.at[c, 6]
            block[...] = term.astype(bf16)
            rs_copy(c, 9, block, ry.at[c], pair).start()
        else:
            rs_copy(c, 9, ry.at[c], ry.at[c], pair).wait_recv()
            proj[c * ROWS : (c + 1) * ROWS] = (term + ry[c].astype(f32)).astype(bf16)

    def rs_drain(c):
        whole, half = terms.at[c, 0], terms.at[c, 0, lo]
        for n in range(10):
            ref = half if n in (1, 2, 5, 6, 7, 8) else whole
            rs_copy(c, n, ref, ref, other).wait_send()
        for h in range(4):
            att_copy(c, h).wait_send()

    block_of = {dest: b for b, dest in enumerate((RING[n % 4], n // 4) for n in range(8))}

    def out_products(c):
        for h in range(4):
            att_copy(c, h).wait_recv()
        events = {
            0: lambda: far_pair(c),
            2: lambda: near_pair(c, 0),
            3: lambda: near_pair(c, 1),
        }
        if c == 0:
            events[4] = lambda: near_free(c, 0)
            events[5] = lambda: near_free(c, 1)

        def one(i):
            b = pick(i, [block_of[dest] for dest in DESTS])
            term = None
            for owner in range(2):
                rows = jnp.concatenate([att[c, owner, h] for h in range(4)], axis=1)
                here = jnp.dot(rows, wo[owner, b], preferred_element_type=f32)
                term = here if term is None else term + here
            terms[c, i] = term.astype(bf16)
            for n, action in events.items():
                when(i, n, action)

        each(0, 8, one)

    def gather_event(n):
        if n == 2:
            g.from_sides(0)
        if n == 4:
            g.from_pair(0)
        if n == 5:
            g.from_far(0)
        if n == 6:
            g.pass_on(1)
            g.pass_pair(0)
            g.from_pair(1)
            g.pass_pair(1)
            g.from_sides(1)
        if n == 9:
            g.from_far(1)
        if n == 10:
            g.from_last(0)
        if n == 11:
            g.from_pair_sides(0)
        if n == 13:
            g.from_last(1)
        if n == 14:
            g.from_pair_sides(1)

    def steps(first, last):
        def one(i):
            for n in (2, 4, 5, 6, 9, 10, 11, 13, 14):
                if first <= n < last:
                    when(i, n, functools.partial(gather_event, n))
            code = pick(i - first, [c * 8 + b for c, b in PLAN[first:last]])
            c, b = code // 8, code % 8

            def ready():
                wq_copy(b).wait()
                wq_across(b).wait_recv()

            if any(c == 0 for c, b in PLAN[first:last]):
                pl.when(c == 0)(ready)
            project(c, b)

        each(first, last, one)

    g.pass_on(0)
    g.start_ring(1)
    wk_copy.wait()
    wv_copy.wait()
    wk_across.wait_recv()
    wv_across.wait_recv()
    steps(0, 13)
    send_partials(0)
    finish_kv(0)
    finish_q(0)
    steps(13, 14)
    kv.pass_on(0)
    steps(14, 16)
    send_partials(1)
    kv.from_sides(0)
    kv.from_pair(0)
    kv.pass_pair(0)
    finish_kv(1)
    kv.from_far(0)
    finish_q(1)
    kv.from_pair_sides(0)
    kv.pass_on(1)
    kv.from_last(0)
    kv.from_sides(1)
    kv.from_pair(1)
    kv.pass_pair(1)
    landed(0, 0, 8)
    kv.from_far(1)
    g.drain(0)
    g.drain(1)
    unit(0, 0, 0, 8, True, False, (None, lambda: kv.from_pair_sides(1), None, lambda: kv.from_last(1)))
    landed(1, 0, 4)
    unit(0, 1, 0, 4, False, False)
    landed(1, 4, 8)
    unit(0, 1, 4, 8, False, True)
    for b in range(8):
        wo_copy(b).wait()
        wo_across(b).wait_recv()
    out_products(0)
    unit(1, 0, 0, 8, True, False)
    here_in(0, 1)
    unit(1, 1, 0, 4, False, False)
    unit(1, 1, 4, 8, False, True, (lambda: far_out(0),))
    out_products(1)
    near_joined(0, 0)
    near_joined(0, 1)
    far_out(1)
    near_free(1, 0)
    near_free(1, 1)
    here_in(1, 1)
    here_in(0, 0)
    near_joined(1, 0)
    near_joined(1, 1)
    for b in range(8):
        wq_across(b).wait_send()
        wo_across(b).wait_send()
    wk_across.wait_send()
    wv_across.wait_send()
    for c in range(2):
        partial_copy(c, 0).wait_send()
        partial_copy(c, 1).wait_send()
        kv.drain(c)
    rs_drain(0)
    here_in(1, 0)
    rs_drain(1)


def hand_over(proj, norm, proj_out, norm_out):
    proj_out[...] = proj[...]
    norm_out[...] = norm[...]


def shards(
    checkpoint, norm_gain, query_weight, key_weight, value_weight, output_weight, block_order
):
    vmem = pl.BlockSpec(memory_space=pltpu.VMEM)
    hbm = pl.BlockSpec(memory_space=pl.ANY)
    dma = pltpu.SemaphoreType.DMA
    shapes = (
        jax.ShapeDtypeStruct((2 * ROWS, FEAT), bf16),
        jax.ShapeDtypeStruct((4, 2 * ROWS), f32),
    )
    results = pl.pallas_call(
        kernel,
        out_shape=shapes,
        in_specs=[pl.BlockSpec(memory_space=pltpu.SMEM), hbm, vmem, hbm, hbm, hbm, hbm],
        out_specs=(vmem, vmem),
        scratch_shapes=[
            pltpu.VMEM((2, 8, ROWS, FEAT), bf16),
            pltpu.VMEM((2, 8, FEAT, FEAT), bf16),
            pltpu.VMEM((2 * HEAD, D), bf16),
            pltpu.VMEM((2, 8, FEAT, FEAT), bf16),
            pltpu.VMEM((2, 2, ROWS, FEAT), f32),
            pltpu.VMEM((2, ROWS, 2 * HEAD), f32),
            pltpu.VMEM((2, ROWS, HEAD), f32),
            pltpu.VMEM((2, ROWS, 2 * HEAD), f32),
            pltpu.VMEM((2, ROWS, FEAT), f32),
            pltpu.VMEM((2, ROWS, 2 * HEAD), f32),
            pltpu.VMEM((2, ROWS, HEAD), f32),
            pltpu.VMEM((2, ROWS, HEAD), f32),
            pltpu.VMEM((2, 4, ROWS, HEAD), bf16),
            pltpu.VMEM((2, 2, N_CP, ROWS, HEAD), bf16),
            pltpu.VMEM((2, N_CP, HEAD, ROWS), bf16),
            pltpu.VMEM((2, N_CP * ROWS, 2 * HEAD), bf16),
            pltpu.VMEM((ROWS, N_CP * ROWS), f32),
            pltpu.VMEM((ROWS, N_CP * ROWS), f32),
            pltpu.VMEM((2, 4, ROWS, HEAD), f32),
            pltpu.VMEM((2, 4, ROWS, 2 * HEAD), f32),
            pltpu.VMEM((2, 2, 4, ROWS, HEAD), bf16),
            pltpu.VMEM((3, ROWS, ROWS), f32),
            pltpu.VMEM((2, 8, ROWS, FEAT), bf16),
            pltpu.VMEM((2, HALF, FEAT), bf16),
            pltpu.VMEM((2, HALF, FEAT), bf16),
            pltpu.VMEM((2, 2, ROWS, FEAT), bf16),
            pltpu.VMEM((2, 2, ROWS, FEAT), bf16),
            pltpu.VMEM((2, ROWS, FEAT), bf16),
            pltpu.VMEM((2, ROWS, FEAT), bf16),
            dma((2,)),
            dma((18,)),
            dma((22,)),
            dma((22,)),
            dma((20,)),
            dma((20,)),
            dma((36,)),
            dma((36,)),
            dma((8,)),
            dma((8,)),
            dma((20,)),
            dma((20,)),
        ],
        compiler_params=pltpu.CompilerParams(
            collective_id=0, has_side_effects=True, vmem_limit_bytes=63000000
        ),
        name="sublayer",
    )(
        block_order,
        checkpoint,
        norm_gain.reshape(D // HEAD, HEAD),
        query_weight,
        key_weight.T,
        value_weight.T,
        output_weight,
    )
    return pl.pallas_call(
        hand_over,
        out_shape=shapes,
        in_specs=[vmem, vmem],
        out_specs=(vmem, vmem),
        name="hand_over",
    )(*results)


def solution(mesh):
    return jax.shard_map(
        shards,
        mesh=mesh,
        in_specs=(
            P("cp", "tp"),
            P(),
            P(None, "tp"),
            P(None, "tp"),
            P(None, "tp"),
            P("tp", None),
            P(),
        ),
        out_specs=(P("cp", "tp"), P("tp", "cp")),
        check_vma=False,
    )
```

```python
import functools
import math

import jax
import jax.numpy as jnp
from jax import lax
from jax.experimental import pallas as pl
from jax.experimental.pallas import tpu as pltpu
from jax.sharding import PartitionSpec as P

MESH = pl.DeviceIdType.MESH
HEAD = 128
ROWS = 256
FEAT = 512
HALF = ROWS // 2
N_TP = 16
N_CP = 8
D = 8192
rope_base = 500000.0
norm_epsilon = 1e-05
masked_score = -1e30
LN2 = math.log(2.0)

f32 = jnp.float32
bf16 = jnp.bfloat16


def pick(i, values):
    out = values[-1]
    for n in range(len(values) - 2, -1, -1):
        out = jnp.where(i == n, values[n], out)
    return out


class Gather:
    def __init__(self, slot, ssem, rsem, right, left, pair, core=None):
        self.slot, self.ssem, self.rsem = slot, ssem, rsem
        self.right, self.left, self.pair, self.core = right, left, pair, core
        self.count = 10 if core is None else 18

    def ref(self, c, b, dk=0, rows=None):
        ref = self.slot(c, b, dk)
        return ref if rows is None else ref.at[pl.ds(rows * HALF, HALF)]

    def copy(self, c, n, ref, device):
        return pltpu.make_async_remote_copy(
            src_ref=ref,
            dst_ref=ref,
            send_sem=self.ssem.at[c * self.count + n],
            recv_sem=self.rsem.at[c * self.count + n],
            device_id=device,
            device_id_type=MESH,
        )

    def send_core(self, c, b):
        if self.core is not None:
            self.copy(c, 10 + b, self.ref(c, b), self.core).start()

    def start_pair(self, c):
        self.copy(c, 8, self.ref(c, 0), self.pair).start()
        self.send_core(c, 0)

    def start_first(self, c):
        self.copy(c, 0, self.ref(c, 0, rows=0), self.right).start()
        self.copy(c, 4, self.ref(c, 0, rows=1), self.left).start()

    def start_second(self, c):
        self.copy(c, 1, self.ref(c, 0, rows=1), self.right).start()
        self.copy(c, 5, self.ref(c, 0, rows=0), self.left).start()

    def pass_on(self, c):
        block = self.ref(c, 1, rows=0)
        self.copy(c, 0, block, self.left).wait_recv()
        self.copy(c, 2, block, self.right).start()
        block = self.ref(c, 2, rows=1)
        self.copy(c, 4, block, self.right).wait_recv()
        self.copy(c, 6, block, self.left).start()

    def from_sides(self, c):
        self.copy(c, 1, self.ref(c, 1, rows=1), self.left).wait_recv()
        self.send_core(c, 1)
        self.copy(c, 5, self.ref(c, 2, rows=0), self.right).wait_recv()
        self.send_core(c, 2)

    def from_pair(self, c):
        self.copy(c, 8, self.ref(c, 4), self.pair).wait_recv()
        self.send_core(c, 4)

    def pass_pair(self, c):
        block = self.ref(c, 4)
        self.copy(c, 3, block, self.right).start()
        self.copy(c, 7, block, self.left).start()

    def from_far(self, c):
        self.copy(c, 2, self.ref(c, 3, rows=0), self.left).wait_recv()
        self.copy(c, 6, self.ref(c, 3, rows=1), self.right).wait_recv()
        self.copy(c, 9, self.ref(c, 3), self.pair).start()
        self.send_core(c, 3)

    def from_pair_sides(self, c):
        self.copy(c, 3, self.ref(c, 5), self.left).wait_recv()
        self.send_core(c, 5)
        self.copy(c, 7, self.ref(c, 6), self.right).wait_recv()
        self.send_core(c, 6)

    def from_last(self, c):
        self.copy(c, 9, self.ref(c, 7), self.pair).wait_recv()
        self.send_core(c, 7)

    def from_core(self, c, b):
        self.copy(c, 10 + b, self.ref(c, b, dk=1), self.core).wait_recv()

    def drain(self, c):
        for n in range(self.count):
            ref = self.ref(c, 0, rows=0 if n in (0, 1, 2, 4, 5, 6) else None)
            self.copy(c, n, ref, self.pair).wait_send()


RING = (0, 3, 1, 2)
KEY_ORDER = (0, 1, 2, 4, 3, 5, 6, 7)
DESTS = ((1, 1), (3, 1), (2, 1), (1, 0), (3, 0), (2, 0), (0, 1), (0, 0))
PLAN = (
    (0, 0), (1, 0), (0, 1), (0, 2), (0, 4), (0, 3), (1, 4), (0, 7), (0, 5), (0, 6),
    (1, 3), (1, 1), (1, 2), (1, 7),
)


def kernel(
    order, x_hbm, gain, wq_hbm, wk_hbm, wv_hbm, wo_hbm,
    proj, norm_out,
    xg, wq, wkv, wo, acc_q, acc_kv, ss, part, part_q, part_kv, cos_t, sin_t, q, kvg, kt, v1,
    scr_a, scr_b, top, outs, att, bias, terms, ra, rb, rc, rd, re, ry,
    x_sem, w_sem, xs, xr, gs, gr, ks, kr, ps, pr, rs, rr,
):
    tp, cp = lax.axis_index("tp"), lax.axis_index("cp")
    core, yh, xx = tp % 2, (tp // 2) % 2, tp // 4
    yl, zz = cp % 2, cp // 2

    def tpi(dr, dp, dk):
        return (((xx + dr) % 4) * 2 + (yh + dp) % 2) * 2 + (core + dk) % 2

    def cpi(dr, dp):
        return ((zz + dr) % 4) * 2 + (yl + dp) % 2

    right, left = {"tp": tpi(1, 0, 0)}, {"tp": tpi(3, 0, 0)}
    pair, other = {"tp": tpi(0, 1, 0)}, {"tp": tpi(0, 0, 1)}
    up, down, beside = {"cp": cpi(1, 0)}, {"cp": cpi(3, 0)}, {"cp": cpi(0, 1)}

    def chip(b):
        dr = RING[b % 4] if isinstance(b, int) else pick(b % 4, RING)
        return ((xx + dr) % 4) * 2 + (yh + b // 4) % 2

    def tp_slot(b, dk):
        return chip(b) * 2 + (core + dk) % 2

    def kv_slot(b):
        dr = RING[b % 4] if isinstance(b, int) else pick(b % 4, RING)
        return cpi(dr, b // 4)

    x_copies = [
        pltpu.make_async_copy(x_hbm.at[pl.ds(c * ROWS, ROWS)], xg.at[c, tp // 2], x_sem.at[c])
        for c in range(2)
    ]
    for copy in x_copies:
        copy.start()

    def features(b, dk):
        return pl.ds(pl.multiple_of(tp_slot(b, dk) * FEAT, FEAT), FEAT)

    def to_other(n, src, dst):
        return pltpu.make_async_remote_copy(
            src_ref=src,
            dst_ref=dst,
            send_sem=xs.at[n],
            recv_sem=xr.at[n],
            device_id=other,
            device_id_type=MESH,
        )

    def wq_copy(b):
        return pltpu.make_async_copy(wq_hbm.at[features(b, 0)], wq.at[0, b], w_sem.at[b])

    def wo_copy(b):
        return pltpu.make_async_copy(wo_hbm.at[:, features(b, 0)], wo.at[0, b], w_sem.at[8 + b])

    def wq_across(b):
        return to_other(b, wq_hbm.at[features(b, 1)], wq.at[1, b])

    def wo_across(b):
        return to_other(8 + b, wo_hbm.at[:, features(b, 1)], wo.at[1, b])

    wk_copy = pltpu.make_async_copy(wk_hbm, wkv.at[pl.ds(0, 64)], w_sem.at[16])
    wv_copy = pltpu.make_async_copy(wv_hbm, wkv.at[pl.ds(64, 64)], w_sem.at[17])
    wk_across = to_other(16, wk_hbm, wkv.at[pl.ds(128, 64)])
    wv_across = to_other(17, wv_hbm, wkv.at[pl.ds(192, 64)])

    barrier = pltpu.get_barrier_semaphore()
    neighbours = (right, left, pair, other, up, down, beside)
    for device in neighbours:
        pl.semaphore_signal(barrier, inc=1, device_id=device, device_id_type=MESH)

    first_use = (0, 1, 2, 4, 3, 7, 5, 6)
    wk_copy.start()
    wv_copy.start()
    for b in first_use:
        wq_copy(b).start()
    for b in range(8):
        wo_copy(b).start()

    pl.semaphore_wait(barrier, len(neighbours))

    g = Gather(lambda c, b, dk: xg.at[c, chip(b)], gs, gr, right, left, pair)
    kv = Gather(
        lambda c, b, dk: kvg.at[c, (core + dk) % 2, kv_slot(b)], ks, kr, up, down, beside, other
    )

    x_copies[0].wait()
    g.start_pair(0)
    g.start_first(0)
    g.start_second(0)
    x_copies[1].wait()
    g.start_pair(1)
    wk_across.start()
    wv_across.start()
    for b in first_use:
        wq_across(b).start()
    for b in range(8):
        wo_across(b).start()

    row_id = lax.broadcasted_iota(jnp.int32, (ROWS, ROWS), 0)
    col_id = lax.broadcasted_iota(jnp.int32, (ROWS, ROWS), 1)
    bias[0] = jnp.zeros((ROWS, ROWS), f32)
    bias[1] = jnp.where(col_id <= row_id, 0.0, masked_score).astype(f32)
    bias[2] = jnp.full((ROWS, ROWS), masked_score, f32)
    acc_q[...] = jnp.zeros_like(acc_q)
    acc_kv[...] = jnp.zeros_like(acc_kv)
    ss[...] = jnp.zeros_like(ss)

    even = (lax.broadcasted_iota(jnp.int32, (ROWS, HEAD), 1) % 2) == 0
    low = lax.broadcasted_iota(jnp.int32, (ROWS, HEAD), 1) < 64

    def make_tables():
        lane8 = lax.broadcasted_iota(jnp.int32, (8, HEAD), 1)
        rate8 = jnp.exp2((lane8 // 2).astype(f32) * (-2.0 / HEAD * math.log2(rope_base)))
        rate = jnp.broadcast_to(rate8[:1], (ROWS, HEAD))
        angle = lax.broadcasted_iota(jnp.int32, (ROWS, HEAD), 0).astype(f32) * rate
        cos_r, sin_r = jnp.cos(angle), jnp.sin(angle)
        sign = jnp.where(even, -1.0, 1.0).astype(f32)
        for c in range(2):
            start = (order[2 * cp + c] * ROWS).astype(f32) * rate8
            cos_b, sin_b = jnp.cos(start)[:1], jnp.sin(start)[:1]
            cos_t[c] = cos_b * cos_r - sin_b * sin_r
            sin_t[c] = (sin_b * cos_r + cos_b * sin_r) * sign

    make_tables()

    def scaled_block(c, b):
        wide = xg[c, chip(b)].astype(f32)
        j = tp_slot(b, 0)
        pieces = [
            (wide[:, n * HEAD : (n + 1) * HEAD] * gain[pl.ds(4 * j + n, 1), :]).astype(bf16)
            for n in range(4)
        ]
        return wide, jnp.concatenate(pieces, axis=1)

    def project_kv(c, b, wide, scaled):
        square = wide * wide
        ss[c] += square[:, :128] + square[:, 128:256] + square[:, 256:384] + square[:, 384:]
        acc_kv[c] += lax.dot_general(
            scaled, wkv[:, features(b, 0)], (((1,), (1,)), ((), ())), preferred_element_type=f32
        )

    def project_q(c, b, scaled):
        for owner in range(2):
            acc_q[c, owner] += jnp.dot(scaled, wq[owner, b], preferred_element_type=f32)

    def project(c, b):
        wide, scaled = scaled_block(c, b)
        project_kv(c, b, wide, scaled)
        project_q(c, b, scaled)

    def partial_copy(c, n):
        if n == 0:
            return to_other(18 + c, part.at[c], part_kv.at[c])
        return to_other(20 + c, acc_q.at[c, 1], part_q.at[c])

    def send_partials(c):
        part[c, :, :HEAD] = acc_kv[c, :, HEAD:]
        part[c, :, HEAD:] = ss[c]
        partial_copy(c, 0).start()

    def turn(y, cosine, sine):
        swapped = jnp.where(even, pltpu.roll(y, HEAD - 1, 1), pltpu.roll(y, 1, 1))
        return y * cosine + swapped * sine

    def finish_kv(c):
        partial_copy(c, 0).wait_recv()
        squares = jnp.sum(ss[c] + part_kv[c, :, HEAD:], axis=1, keepdims=True)
        scale = jnp.broadcast_to(lax.rsqrt(squares * (1.0 / D) + norm_epsilon), (ROWS, HEAD))
        ss[c] = scale
        cosine, sine = cos_t[c], sin_t[c]
        k_cos = jnp.where(core == 0, cosine, pltpu.roll(cosine, 64, 1))
        k_sin = jnp.where(core == 0, sine, pltpu.roll(sine, 64, 1))
        k_cos, k_sin = jnp.where(low, k_cos, 1.0), jnp.where(low, k_sin, 0.0)
        both = (acc_kv[c, :, :HEAD] + part_kv[c, :, :HEAD]) * scale
        kvg[c, core, cp] = turn(both, k_cos, k_sin).astype(bf16)
        kv.start_pair(c)
        kv.start_first(c)
        kv.start_second(c)

    def finish_q(c):
        partial_copy(c, 1).wait_recv()
        cosine, sine = cos_t[c], sin_t[c]
        q_scale = ss[c] * (math.log2(math.e) / math.sqrt(HEAD))
        for h in range(4):
            lanes = slice(h * HEAD, (h + 1) * HEAD)
            y = (acc_q[c, 0, :, lanes] + part_q[c, :, lanes]) * q_scale
            q[c, h] = turn(y, cosine, sine).astype(bf16)

    def each(first, last, body):
        def one(i, unused):
            body(i)
            return unused

        lax.fori_loop(first, last, one, 0)

    def when(i, n, action):
        pl.when(i == n)(action)

    def assemble(c, p):
        slot = kv_slot(pick(p, KEY_ORDER))
        lower, upper = kvg[c, 0, slot].astype(f32), kvg[c, 1, slot].astype(f32)
        keys = jnp.where(low, lower, pltpu.roll(upper, 64, 1))
        values = jnp.where(low, pltpu.roll(lower, 64, 1), upper)
        kt[c, p] = keys.T.astype(bf16)
        rows = pl.ds(pl.multiple_of(p * ROWS, ROWS), ROWS)
        v1[c, rows, :HEAD] = values.astype(bf16)
        v1[c, rows, HEAD:] = jnp.ones((ROWS, HEAD), bf16)

    def landed(c, first, last):
        for b in KEY_ORDER[first:last]:
            kv.from_core(c, b)
        each(first, last, functools.partial(assemble, c))

    def unit(qc, kc, start, stop, first, last, between=()):
        q_block = order[2 * cp + qc]
        which = {}
        for p in range(start, stop):
            k_block = order[2 * kv_slot(KEY_ORDER[p]) + kc]
            which[p] = jnp.where(k_block < q_block, 0, jnp.where(k_block == q_block, 1, 2))
        group = 4
        tops = {}

        def score(h, p, best):
            scr = (scr_a, scr_b)[h % 2]
            scores = jnp.dot(q[qc, h], kt[kc, p], preferred_element_type=f32) + bias[which[p]]
            scr[:, p * ROWS : (p + 1) * ROWS] = scores
            here = jnp.maximum(scores[:, :HEAD], scores[:, HEAD:])
            return here if best is None else jnp.maximum(best, here)

        def settle(h, best):
            new_top = jnp.broadcast_to(jnp.max(best, axis=1, keepdims=True), (ROWS, HEAD))
            tops[h] = new_top if first else jnp.maximum(top[qc, h], new_top)

        def weigh(h, p, total):
            scr = (scr_a, scr_b)[h % 2]
            both = jnp.concatenate([tops[h]] * 2, axis=1)
            weights = [
                jnp.exp2(scr[:, n * ROWS : (n + 1) * ROWS] - both).astype(bf16)
                for n in range(p, p + group)
            ]
            here = jnp.dot(
                jnp.concatenate(weights, axis=1),
                v1[kc, p * ROWS : (p + group) * ROWS],
                preferred_element_type=f32,
            )
            return here if total is None else total + here

        def close(h, total):
            if not first:
                shrink = jnp.exp2(top[qc, h] - tops[h])
                total = total + outs[qc, h] * jnp.concatenate([shrink, shrink], axis=1)
            if last:
                sums = total[:, HEAD:]
                att[qc, 0, h] = (total[:, :HEAD] / sums).astype(bf16)
                att_copy(qc, h).start()
                normalizer = (tops[h] + jnp.log2(sums)) * LN2
                norm_out[h : h + 1, qc * ROWS : (qc + 1) * ROWS] = normalizer.T[:1]
            else:
                top[qc, h] = tops[h]
                outs[qc, h] = total

        best = None
        for p in range(start, stop):
            best = score(0, p, best)
        settle(0, best)
        for h in range(4):
            best = total = None
            for p in range(start, stop):
                if h < 3:
                    best = score(h + 1, p, best)
                if p % group == group - 1:
                    total = weigh(h, p - group + 1, total)
            close(h, total)
            if h < 3:
                settle(h + 1, best)
            if h < len(between) and between[h] is not None:
                between[h]()

    def att_copy(c, h):
        return pltpu.make_async_remote_copy(
            src_ref=att.at[c, 0, h],
            dst_ref=att.at[c, 1, h],
            send_sem=ps.at[c * 4 + h],
            recv_sem=pr.at[c * 4 + h],
            device_id=other,
            device_id_type=MESH,
        )

    def rs_copy(c, n, src, dst, device):
        return pltpu.make_async_remote_copy(
            src_ref=src,
            dst_ref=dst,
            send_sem=rs.at[c * 10 + n],
            recv_sem=rr.at[c * 10 + n],
            device_id=device,
            device_id_type=MESH,
        )

    lo, hi = pl.ds(0, HALF), pl.ds(HALF, HALF)
    ways = (right, left)

    def far_pair(c):
        rs_copy(c, 0, terms.at[c, 2], re.at[c], pair).start()

    def far_out(c):
        block = terms.at[c, 5]
        rs_copy(c, 0, re.at[c], re.at[c], pair).wait_recv()
        block[...] = (block[...].astype(f32) + re[c].astype(f32)).astype(bf16)
        rs_copy(c, 1, block.at[lo], ra.at[c], right).start()
        rs_copy(c, 2, block.at[hi], rb.at[c], left).start()

    def near_pair(c, side):
        rs_copy(c, 3 + side, terms.at[c, side], (rc, rd)[side].at[c, 1], ways[side]).start()

    def near_free(c, side):
        half = (hi, lo)[side]
        rs_copy(
            c, 5 + side, terms.at[c, 3 + side].at[half], (rc, rd)[side].at[c, 0].at[half], ways[side]
        ).start()

    def near_joined(c, side):
        half = (lo, hi)[side]
        block, moved = terms.at[c, 3 + side].at[half], (ra, rb)[side].at[c]
        rs_copy(c, 1 + side, moved, moved, left).wait_recv()
        block[...] = (block[...].astype(f32) + moved[...].astype(f32)).astype(bf16)
        rs_copy(c, 7 + side, block, (rc, rd)[side].at[c, 0].at[half], ways[side]).start()

    def here_in(c, p):
        term = terms[c, 7 - p].astype(f32)
        for side in range(2):
            block = (rc, rd)[side].at[c, p]
            if p == 1:
                rs_copy(c, 3 + side, block, block, left).wait_recv()
            else:
                for n, half in ((5, (hi, lo)[side]), (7, (lo, hi)[side])):
                    rs_copy(c, n + side, block.at[half], block.at[half], left).wait_recv()
            term = term + block[...].astype(f32)
        if p == 1:
            block = terms.at[c, 6]
            block[...] = term.astype(bf16)
            rs_copy(c, 9, block, ry.at[c], pair).start()
        else:
            rs_copy(c, 9, ry.at[c], ry.at[c], pair).wait_recv()
            proj[c * ROWS : (c + 1) * ROWS] = (term + ry[c].astype(f32)).astype(bf16)

    def rs_drain(c):
        whole, half = terms.at[c, 0], terms.at[c, 0, lo]
        for n in range(10):
            ref = half if n in (1, 2, 5, 6, 7, 8) else whole
            rs_copy(c, n, ref, ref, other).wait_send()
        for h in range(4):
            att_copy(c, h).wait_send()

    block_of = {dest: b for b, dest in enumerate((RING[n % 4], n // 4) for n in range(8))}

    def out_products(c):
        for h in range(4):
            att_copy(c, h).wait_recv()
        events = {
            0: lambda: near_pair(c, 0),
            1: lambda: near_pair(c, 1),
            2: lambda: far_pair(c),
        }
        if c == 0:
            events[3] = lambda: near_free(c, 0)
            events[4] = lambda: near_free(c, 1)

        def one(i):
            b = pick(i, [block_of[dest] for dest in DESTS])
            term = None
            for owner in range(2):
                rows = jnp.concatenate([att[c, owner, h] for h in range(4)], axis=1)
                here = jnp.dot(rows, wo[owner, b], preferred_element_type=f32)
                term = here if term is None else term + here
            terms[c, i] = term.astype(bf16)
            for n, action in events.items():
                when(i, n, action)

        each(0, 8, one)

    def gather_event(n):
        if n == 2:
            g.from_sides(0)
        if n == 4:
            g.from_pair(0)
            g.pass_pair(0)
        if n == 5:
            g.from_far(0)
        if n == 6:
            g.pass_on(1)
            g.start_second(1)
            g.from_pair(1)
            g.pass_pair(1)
        if n == 7:
            g.from_last(0)
        if n == 8:
            g.from_pair_sides(0)
        if n == 11:
            kv.pass_on(0)
            g.from_sides(1)
        if n == 13:
            kv.from_sides(0)
            kv.from_pair(0)
            kv.pass_pair(0)
            kv.from_far(0)
            kv.from_pair_sides(0)
            g.from_last(1)

    def steps(first, last):
        def one(i):
            for n in (2, 4, 5, 6, 7, 8, 11, 13):
                if first <= n < last:
                    when(i, n, functools.partial(gather_event, n))
            code = pick(i - first, [c * 8 + b for c, b in PLAN[first:last]])
            c, b = code // 8, code % 8

            def ready():
                wq_copy(b).wait()
                wq_across(b).wait_recv()

            if any(c == 0 for c, b in PLAN[first:last]):
                pl.when(c == 0)(ready)
            project(c, b)

        each(first, last, one)

    g.pass_on(0)
    g.start_first(1)
    wk_copy.wait()
    wv_copy.wait()
    wk_across.wait_recv()
    wv_across.wait_recv()
    steps(0, 10)
    send_partials(0)
    partial_copy(0, 1).start()
    finish_kv(0)
    g.from_far(1)
    finish_q(0)
    steps(10, 14)
    kv.from_last(0)
    landed(0, 0, 4)
    g.from_pair_sides(1)
    late = [scaled_block(1, b) for b in (5, 6)]
    for b, (wide, scaled) in zip((5, 6), late):
        project_kv(1, b, wide, scaled)
    send_partials(1)
    for b, (wide, scaled) in zip((5, 6), late):
        project_q(1, b, scaled)
    partial_copy(1, 1).start()
    finish_kv(1)
    landed(0, 4, 8)
    finish_q(1)
    g.drain(0)
    g.drain(1)

    def near_keys():
        kv.from_sides(1)
        kv.from_pair(1)
        kv.pass_pair(1)

    unit(0, 0, 0, 8, True, False, (lambda: kv.pass_on(1), near_keys))
    kv.from_far(1)
    landed(1, 0, 4)
    unit(0, 1, 0, 4, False, False, (None, None, lambda: kv.from_pair_sides(1)))
    kv.from_last(1)
    landed(1, 4, 8)
    unit(0, 1, 4, 8, False, True)
    for b in range(8):
        wo_copy(b).wait()
        wo_across(b).wait_recv()
    out_products(0)
    unit(1, 0, 0, 8, True, False)
    unit(1, 1, 0, 4, False, False)
    unit(1, 1, 4, 8, False, True, (lambda: far_out(0),))
    out_products(1)
    here_in(0, 1)
    near_joined(0, 0)
    near_joined(0, 1)
    far_out(1)
    near_free(1, 0)
    near_free(1, 1)
    here_in(1, 1)
    here_in(0, 0)
    near_joined(1, 0)
    near_joined(1, 1)
    for b in range(8):
        wq_across(b).wait_send()
        wo_across(b).wait_send()
    wk_across.wait_send()
    wv_across.wait_send()
    for c in range(2):
        partial_copy(c, 0).wait_send()
        partial_copy(c, 1).wait_send()
        kv.drain(c)
    rs_drain(0)
    here_in(1, 0)
    rs_drain(1)


def hand_over(proj, norm, proj_out, norm_out):
    proj_out[...] = proj[...]
    norm_out[...] = norm[...]


def shards(
    checkpoint, norm_gain, query_weight, key_weight, value_weight, output_weight, block_order
):
    vmem = pl.BlockSpec(memory_space=pltpu.VMEM)
    hbm = pl.BlockSpec(memory_space=pl.ANY)
    dma = pltpu.SemaphoreType.DMA
    shapes = (
        jax.ShapeDtypeStruct((2 * ROWS, FEAT), bf16),
        jax.ShapeDtypeStruct((4, 2 * ROWS), f32),
    )
    results = pl.pallas_call(
        kernel,
        out_shape=shapes,
        in_specs=[pl.BlockSpec(memory_space=pltpu.SMEM), hbm, vmem, hbm, hbm, hbm, hbm],
        out_specs=(vmem, vmem),
        scratch_shapes=[
            pltpu.VMEM((2, 8, ROWS, FEAT), bf16),
            pltpu.VMEM((2, 8, FEAT, FEAT), bf16),
            pltpu.VMEM((2 * HEAD, D), bf16),
            pltpu.VMEM((2, 8, FEAT, FEAT), bf16),
            pltpu.VMEM((2, 2, ROWS, FEAT), f32),
            pltpu.VMEM((2, ROWS, 2 * HEAD), f32),
            pltpu.VMEM((2, ROWS, HEAD), f32),
            pltpu.VMEM((2, ROWS, 2 * HEAD), f32),
            pltpu.VMEM((2, ROWS, FEAT), f32),
            pltpu.VMEM((2, ROWS, 2 * HEAD), f32),
            pltpu.VMEM((2, ROWS, HEAD), f32),
            pltpu.VMEM((2, ROWS, HEAD), f32),
            pltpu.VMEM((2, 4, ROWS, HEAD), bf16),
            pltpu.VMEM((2, 2, N_CP, ROWS, HEAD), bf16),
            pltpu.VMEM((2, N_CP, HEAD, ROWS), bf16),
            pltpu.VMEM((2, N_CP * ROWS, 2 * HEAD), bf16),
            pltpu.VMEM((ROWS, N_CP * ROWS), f32),
            pltpu.VMEM((ROWS, N_CP * ROWS), f32),
            pltpu.VMEM((2, 4, ROWS, HEAD), f32),
            pltpu.VMEM((2, 4, ROWS, 2 * HEAD), f32),
            pltpu.VMEM((2, 2, 4, ROWS, HEAD), bf16),
            pltpu.VMEM((3, ROWS, ROWS), f32),
            pltpu.VMEM((2, 8, ROWS, FEAT), bf16),
            pltpu.VMEM((2, HALF, FEAT), bf16),
            pltpu.VMEM((2, HALF, FEAT), bf16),
            pltpu.VMEM((2, 2, ROWS, FEAT), bf16),
            pltpu.VMEM((2, 2, ROWS, FEAT), bf16),
            pltpu.VMEM((2, ROWS, FEAT), bf16),
            pltpu.VMEM((2, ROWS, FEAT), bf16),
            dma((2,)),
            dma((18,)),
            dma((22,)),
            dma((22,)),
            dma((20,)),
            dma((20,)),
            dma((36,)),
            dma((36,)),
            dma((8,)),
            dma((8,)),
            dma((20,)),
            dma((20,)),
        ],
        compiler_params=pltpu.CompilerParams(
            collective_id=0, has_side_effects=True, vmem_limit_bytes=63000000
        ),
        name="sublayer",
    )(
        block_order,
        checkpoint,
        norm_gain.reshape(D // HEAD, HEAD),
        query_weight,
        key_weight.T,
        value_weight.T,
        output_weight,
    )
    return pl.pallas_call(
        hand_over,
        out_shape=shapes,
        in_specs=[vmem, vmem],
        out_specs=(vmem, vmem),
        name="hand_over",
    )(*results)


def solution(mesh):
    return jax.shard_map(
        shards,
        mesh=mesh,
        in_specs=(
            P("cp", "tp"),
            P(),
            P(None, "tp"),
            P(None, "tp"),
            P(None, "tp"),
            P("tp", None),
            P(),
        ),
        out_specs=(P("cp", "tp"), P("tp", "cp")),
        check_vma=False,
    )
```

```python
import functools
import math

import jax
import jax.numpy as jnp
from jax import lax
from jax.experimental import pallas as pl
from jax.experimental.pallas import tpu as pltpu
from jax.sharding import PartitionSpec as P

MESH = pl.DeviceIdType.MESH
HEAD = 128
ROWS = 256
FEAT = 512
HALF = ROWS // 2
N_TP = 16
N_CP = 8
D = 8192
rope_base = 500000.0
norm_epsilon = 1e-05
masked_score = -1e30
LN2 = math.log(2.0)

f32 = jnp.float32
bf16 = jnp.bfloat16


def pick(i, values):
    out = values[-1]
    for n in range(len(values) - 2, -1, -1):
        out = jnp.where(i == n, values[n], out)
    return out


class Gather:
    def __init__(self, slot, ssem, rsem, right, left, pair, core=None):
        self.slot, self.ssem, self.rsem = slot, ssem, rsem
        self.right, self.left, self.pair, self.core = right, left, pair, core
        self.count = 10 if core is None else 18

    def ref(self, c, b, dk=0, rows=None):
        ref = self.slot(c, b, dk)
        return ref if rows is None else ref.at[pl.ds(rows * HALF, HALF)]

    def copy(self, c, n, ref, device):
        return pltpu.make_async_remote_copy(
            src_ref=ref,
            dst_ref=ref,
            send_sem=self.ssem.at[c * self.count + n],
            recv_sem=self.rsem.at[c * self.count + n],
            device_id=device,
            device_id_type=MESH,
        )

    def send_core(self, c, b):
        if self.core is not None:
            self.copy(c, 10 + b, self.ref(c, b), self.core).start()

    def start_pair(self, c):
        self.copy(c, 8, self.ref(c, 0), self.pair).start()
        self.send_core(c, 0)

    def start_first(self, c):
        self.copy(c, 0, self.ref(c, 0, rows=0), self.right).start()
        self.copy(c, 4, self.ref(c, 0, rows=1), self.left).start()

    def start_second(self, c):
        self.copy(c, 1, self.ref(c, 0, rows=1), self.right).start()
        self.copy(c, 5, self.ref(c, 0, rows=0), self.left).start()

    def pass_on(self, c):
        block = self.ref(c, 1, rows=0)
        self.copy(c, 0, block, self.left).wait_recv()
        self.copy(c, 2, block, self.right).start()
        block = self.ref(c, 2, rows=1)
        self.copy(c, 4, block, self.right).wait_recv()
        self.copy(c, 6, block, self.left).start()

    def from_sides(self, c):
        self.copy(c, 1, self.ref(c, 1, rows=1), self.left).wait_recv()
        self.send_core(c, 1)
        self.copy(c, 5, self.ref(c, 2, rows=0), self.right).wait_recv()
        self.send_core(c, 2)

    def from_pair(self, c):
        self.copy(c, 8, self.ref(c, 4), self.pair).wait_recv()
        self.send_core(c, 4)

    def pass_pair(self, c):
        block = self.ref(c, 4)
        self.copy(c, 3, block, self.right).start()
        self.copy(c, 7, block, self.left).start()

    def from_far(self, c):
        self.copy(c, 2, self.ref(c, 3, rows=0), self.left).wait_recv()
        self.copy(c, 6, self.ref(c, 3, rows=1), self.right).wait_recv()
        self.copy(c, 9, self.ref(c, 3), self.pair).start()
        self.send_core(c, 3)

    def from_pair_sides(self, c):
        self.copy(c, 3, self.ref(c, 5), self.left).wait_recv()
        self.send_core(c, 5)
        self.copy(c, 7, self.ref(c, 6), self.right).wait_recv()
        self.send_core(c, 6)

    def from_last(self, c):
        self.copy(c, 9, self.ref(c, 7), self.pair).wait_recv()
        self.send_core(c, 7)

    def from_core(self, c, b):
        self.copy(c, 10 + b, self.ref(c, b, dk=1), self.core).wait_recv()

    def drain(self, c):
        for n in range(self.count):
            ref = self.ref(c, 0, rows=0 if n in (0, 1, 2, 4, 5, 6) else None)
            self.copy(c, n, ref, self.pair).wait_send()


RING = (0, 3, 1, 2)
KEY_ORDER = (0, 1, 2, 4, 3, 5, 6, 7)
DESTS = ((1, 1), (3, 1), (2, 1), (1, 0), (3, 0), (2, 0), (0, 1), (0, 0))
PLAN = (
    (0, 0), (1, 0), (0, 1), (0, 2), (0, 4), (0, 3), (1, 4), (0, 7), (0, 5), (0, 6),
    (1, 3), (1, 1), (1, 2), (1, 7),
)


def kernel(
    order, x_hbm, gain, wq_hbm, wk_hbm, wv_hbm, wo_hbm,
    proj, norm_out,
    xg, wq, wkv, wo, acc_q, acc_kv, ss, part, part_q, part_kv, cos_t, sin_t, q, kvg,
    scr_a, scr_b, top, outs, att, bias, terms, ra, rb, rc, rd, re, ry,
    x_sem, w_sem, xs, xr, gs, gr, ks, kr, ps, pr, rs, rr,
):
    tp, cp = lax.axis_index("tp"), lax.axis_index("cp")
    core, yh, xx = tp % 2, (tp // 2) % 2, tp // 4
    yl, zz = cp % 2, cp // 2

    def tpi(dr, dp, dk):
        return (((xx + dr) % 4) * 2 + (yh + dp) % 2) * 2 + (core + dk) % 2

    def cpi(dr, dp):
        return ((zz + dr) % 4) * 2 + (yl + dp) % 2

    right, left = {"tp": tpi(1, 0, 0)}, {"tp": tpi(3, 0, 0)}
    pair, other = {"tp": tpi(0, 1, 0)}, {"tp": tpi(0, 0, 1)}
    up, down, beside = {"cp": cpi(1, 0)}, {"cp": cpi(3, 0)}, {"cp": cpi(0, 1)}

    def chip(b):
        dr = RING[b % 4] if isinstance(b, int) else pick(b % 4, RING)
        return ((xx + dr) % 4) * 2 + (yh + b // 4) % 2

    def tp_slot(b, dk):
        return chip(b) * 2 + (core + dk) % 2

    def kv_slot(b):
        dr = RING[b % 4] if isinstance(b, int) else pick(b % 4, RING)
        return cpi(dr, b // 4)

    x_copies = [
        pltpu.make_async_copy(x_hbm.at[pl.ds(c * ROWS, ROWS)], xg.at[c, tp // 2], x_sem.at[c])
        for c in range(2)
    ]
    for copy in x_copies:
        copy.start()

    def features(b, dk):
        return pl.ds(pl.multiple_of(tp_slot(b, dk) * FEAT, FEAT), FEAT)

    def to_other(n, src, dst):
        return pltpu.make_async_remote_copy(
            src_ref=src,
            dst_ref=dst,
            send_sem=xs.at[n],
            recv_sem=xr.at[n],
            device_id=other,
            device_id_type=MESH,
        )

    def wq_copy(b):
        return pltpu.make_async_copy(wq_hbm.at[features(b, 0)], wq.at[0, b], w_sem.at[b])

    def wo_copy(b):
        return pltpu.make_async_copy(wo_hbm.at[:, features(b, 0)], wo.at[0, b], w_sem.at[8 + b])

    def wq_across(b):
        return to_other(b, wq_hbm.at[features(b, 1)], wq.at[1, b])

    def wo_across(b):
        return to_other(8 + b, wo_hbm.at[:, features(b, 1)], wo.at[1, b])

    outer = pl.ds(pl.multiple_of(192 * core, 64), 64)
    inner = pl.ds(pl.multiple_of(128 - 64 * core, 64), 64)
    wk_copy = pltpu.make_async_copy(wk_hbm, wkv.at[outer], w_sem.at[16])
    wv_copy = pltpu.make_async_copy(wv_hbm, wkv.at[inner], w_sem.at[17])
    wk_across = to_other(16, wk_hbm, wkv.at[inner])
    wv_across = to_other(17, wv_hbm, wkv.at[outer])

    barrier = pltpu.get_barrier_semaphore()
    neighbours = (right, left, pair, other, up, down, beside)
    for device in neighbours:
        pl.semaphore_signal(barrier, inc=1, device_id=device, device_id_type=MESH)

    first_use = (0, 1, 2, 4, 3, 7, 5, 6)
    wk_copy.start()
    wv_copy.start()
    for b in first_use:
        wq_copy(b).start()
    for b in range(8):
        wo_copy(b).start()

    pl.semaphore_wait(barrier, len(neighbours))

    g = Gather(lambda c, b, dk: xg.at[c, chip(b)], gs, gr, right, left, pair)
    kv = Gather(
        lambda c, b, dk: kvg.at[c, (core + dk) % 2, kv_slot(b)], ks, kr, up, down, beside, other
    )

    x_copies[0].wait()
    g.start_pair(0)
    g.start_first(0)
    g.start_second(0)
    x_copies[1].wait()
    g.start_pair(1)
    wk_across.start()
    wv_across.start()
    for b in first_use:
        wq_across(b).start()
    for b in range(8):
        wo_across(b).start()

    row_id = lax.broadcasted_iota(jnp.int32, (ROWS, ROWS), 0)
    col_id = lax.broadcasted_iota(jnp.int32, (ROWS, ROWS), 1)
    bias[0] = jnp.zeros((ROWS, ROWS), f32)
    bias[1] = jnp.where(col_id <= row_id, 0.0, masked_score).astype(f32)
    bias[2] = jnp.full((ROWS, ROWS), masked_score, f32)
    acc_q[...] = jnp.zeros_like(acc_q)
    acc_kv[...] = jnp.zeros_like(acc_kv)
    ss[...] = jnp.zeros_like(ss)

    even = (lax.broadcasted_iota(jnp.int32, (ROWS, HEAD), 1) % 2) == 0

    def make_tables():
        lane8 = lax.broadcasted_iota(jnp.int32, (8, HEAD), 1)
        rate8 = jnp.exp2((lane8 // 2).astype(f32) * (-2.0 / HEAD * math.log2(rope_base)))
        rate = jnp.broadcast_to(rate8[:1], (ROWS, HEAD))
        angle = lax.broadcasted_iota(jnp.int32, (ROWS, HEAD), 0).astype(f32) * rate
        cos_r, sin_r = jnp.cos(angle), jnp.sin(angle)
        sign = jnp.where(even, -1.0, 1.0).astype(f32)
        for c in range(2):
            start = (order[2 * cp + c] * ROWS).astype(f32) * rate8
            cos_b, sin_b = jnp.cos(start)[:1], jnp.sin(start)[:1]
            cos_t[c] = cos_b * cos_r - sin_b * sin_r
            sin_t[c] = (sin_b * cos_r + cos_b * sin_r) * sign

    make_tables()

    def scaled_block(c, b):
        wide = xg[c, chip(b)].astype(f32)
        j = tp_slot(b, 0)
        pieces = [
            (wide[:, n * HEAD : (n + 1) * HEAD] * gain[pl.ds(4 * j + n, 1), :]).astype(bf16)
            for n in range(4)
        ]
        return wide, jnp.concatenate(pieces, axis=1)

    def project_kv(c, b, wide, scaled):
        square = wide * wide
        ss[c] += square[:, :128] + square[:, 128:256] + square[:, 256:384] + square[:, 384:]
        acc_kv[c] += lax.dot_general(
            scaled, wkv[:, features(b, 0)], (((1,), (1,)), ((), ())), preferred_element_type=f32
        )

    def project_q(c, b, scaled):
        for owner in range(2):
            acc_q[c, owner] += jnp.dot(scaled, wq[owner, b], preferred_element_type=f32)

    def project(c, b):
        wide, scaled = scaled_block(c, b)
        project_kv(c, b, wide, scaled)
        project_q(c, b, scaled)

    def partial_copy(c, n):
        if n == 0:
            return to_other(18 + c, part.at[c], part_kv.at[c])
        return to_other(20 + c, acc_q.at[c, 1], part_q.at[c])

    def send_partials(c):
        part[c, :, :HEAD] = acc_kv[c, :, HEAD:]
        part[c, :, HEAD:] = ss[c]
        partial_copy(c, 0).start()

    def turn(y, cosine, sine):
        swapped = jnp.where(even, pltpu.roll(y, HEAD - 1, 1), pltpu.roll(y, 1, 1))
        return y * cosine + swapped * sine

    def finish_kv(c):
        partial_copy(c, 0).wait_recv()
        squares = jnp.sum(ss[c] + part_kv[c, :, HEAD:], axis=1, keepdims=True)
        scale = jnp.broadcast_to(lax.rsqrt(squares * (1.0 / D) + norm_epsilon), (ROWS, HEAD))
        ss[c] = scale
        cosine, sine = cos_t[c], sin_t[c]
        both = (acc_kv[c, :, :HEAD] + part_kv[c, :, :HEAD]) * scale
        turned = turn(both, cosine, sine)
        keys = jnp.concatenate([turned[:HALF].T, turned[HALF:].T], axis=0)
        kvg[c, core, cp] = jnp.where(core == 0, keys, both).astype(bf16)
        kv.start_pair(c)
        kv.start_first(c)
        kv.start_second(c)

    def finish_q(c):
        partial_copy(c, 1).wait_recv()
        cosine, sine = cos_t[c], sin_t[c]
        q_scale = ss[c] * (math.log2(math.e) / math.sqrt(HEAD))
        for h in range(4):
            lanes = slice(h * HEAD, (h + 1) * HEAD)
            y = (acc_q[c, 0, :, lanes] + part_q[c, :, lanes]) * q_scale
            q[c, h] = turn(y, cosine, sine).astype(bf16)

    def each(first, last, body):
        def one(i, unused):
            body(i)
            return unused

        lax.fori_loop(first, last, one, 0)

    def when(i, n, action):
        pl.when(i == n)(action)

    def landed(c, first, last):
        for b in KEY_ORDER[first:last]:
            kv.from_core(c, b)

    def unit(qc, kc, start, stop, first, last, between=()):
        q_block = order[2 * cp + qc]
        which, slots = {}, {}
        for p in range(start, stop):
            slots[p] = kv_slot(KEY_ORDER[p])
            k_block = order[2 * slots[p] + kc]
            which[p] = jnp.where(k_block < q_block, 0, jnp.where(k_block == q_block, 1, 2))
        group = 4
        tops = {}

        def score(h, p, best):
            scr = (scr_a, scr_b)[h % 2]
            halves = [kvg[kc, 0, slots[p], :HALF], kvg[kc, 0, slots[p], HALF:]]
            keys = jnp.concatenate(halves, axis=1)
            scores = jnp.dot(q[qc, h], keys, preferred_element_type=f32) + bias[which[p]]
            scr[:, p * ROWS : (p + 1) * ROWS] = scores
            here = jnp.maximum(scores[:, :HEAD], scores[:, HEAD:])
            return here if best is None else jnp.maximum(best, here)

        def settle(h, best):
            new_top = jnp.broadcast_to(jnp.max(best, axis=1, keepdims=True), (ROWS, HEAD))
            tops[h] = new_top if first else jnp.maximum(top[qc, h], new_top)

        def weigh(h, p, total):
            scr = (scr_a, scr_b)[h % 2]
            both = jnp.concatenate([tops[h]] * 2, axis=1)
            weights = [
                jnp.exp2(scr[:, n * ROWS : (n + 1) * ROWS] - both).astype(bf16)
                for n in range(p, p + group)
            ]
            values = jnp.concatenate([kvg[kc, 1, slots[n]] for n in range(p, p + group)], axis=0)
            here = jnp.dot(
                jnp.concatenate(weights, axis=1),
                jnp.concatenate([values, jnp.ones((group * ROWS, HEAD), bf16)], axis=1),
                preferred_element_type=f32,
            )
            return here if total is None else total + here

        def close(h, total):
            if not first:
                shrink = jnp.exp2(top[qc, h] - tops[h])
                total = total + outs[qc, h] * jnp.concatenate([shrink, shrink], axis=1)
            if last:
                sums = total[:, HEAD:]
                att[qc, 0, h] = (total[:, :HEAD] / sums).astype(bf16)
                att_copy(qc, h).start()
                normalizer = (tops[h] + jnp.log2(sums)) * LN2
                norm_out[h : h + 1, qc * ROWS : (qc + 1) * ROWS] = normalizer.T[:1]
            else:
                top[qc, h] = tops[h]
                outs[qc, h] = total

        best = None
        for p in range(start, stop):
            best = score(0, p, best)
        settle(0, best)
        for h in range(4):
            best = total = None
            for p in range(start, stop):
                if h < 3:
                    best = score(h + 1, p, best)
                if p % group == group - 1:
                    total = weigh(h, p - group + 1, total)
            close(h, total)
            if h < 3:
                settle(h + 1, best)
            if h < len(between) and between[h] is not None:
                between[h]()

    def att_copy(c, h):
        return pltpu.make_async_remote_copy(
            src_ref=att.at[c, 0, h],
            dst_ref=att.at[c, 1, h],
            send_sem=ps.at[c * 4 + h],
            recv_sem=pr.at[c * 4 + h],
            device_id=other,
            device_id_type=MESH,
        )

    def rs_copy(c, n, src, dst, device):
        return pltpu.make_async_remote_copy(
            src_ref=src,
            dst_ref=dst,
            send_sem=rs.at[c * 10 + n],
            recv_sem=rr.at[c * 10 + n],
            device_id=device,
            device_id_type=MESH,
        )

    lo, hi = pl.ds(0, HALF), pl.ds(HALF, HALF)
    ways = (right, left)

    def far_pair(c):
        rs_copy(c, 0, terms.at[c, 2], re.at[c], pair).start()

    def far_out(c):
        block = terms.at[c, 5]
        rs_copy(c, 0, re.at[c], re.at[c], pair).wait_recv()
        block[...] = (block[...].astype(f32) + re[c].astype(f32)).astype(bf16)
        rs_copy(c, 1, block.at[lo], ra.at[c], right).start()
        rs_copy(c, 2, block.at[hi], rb.at[c], left).start()

    def near_pair(c, side):
        rs_copy(c, 3 + side, terms.at[c, side], (rc, rd)[side].at[c, 1], ways[side]).start()

    def near_free(c, side):
        half = (hi, lo)[side]
        rs_copy(
            c, 5 + side, terms.at[c, 3 + side].at[half], (rc, rd)[side].at[c, 0].at[half], ways[side]
        ).start()

    def near_joined(c, side):
        half = (lo, hi)[side]
        block, moved = terms.at[c, 3 + side].at[half], (ra, rb)[side].at[c]
        rs_copy(c, 1 + side, moved, moved, left).wait_recv()
        block[...] = (block[...].astype(f32) + moved[...].astype(f32)).astype(bf16)
        rs_copy(c, 7 + side, block, (rc, rd)[side].at[c, 0].at[half], ways[side]).start()

    def here_in(c, p):
        term = terms[c, 7 - p].astype(f32)
        for side in range(2):
            block = (rc, rd)[side].at[c, p]
            if p == 1:
                rs_copy(c, 3 + side, block, block, left).wait_recv()
            else:
                for n, half in ((5, (hi, lo)[side]), (7, (lo, hi)[side])):
                    rs_copy(c, n + side, block.at[half], block.at[half], left).wait_recv()
            term = term + block[...].astype(f32)
        if p == 1:
            block = terms.at[c, 6]
            block[...] = term.astype(bf16)
            rs_copy(c, 9, block, ry.at[c], pair).start()
        else:
            rs_copy(c, 9, ry.at[c], ry.at[c], pair).wait_recv()
            proj[c * ROWS : (c + 1) * ROWS] = (term + ry[c].astype(f32)).astype(bf16)

    def rs_drain(c):
        whole, half = terms.at[c, 0], terms.at[c, 0, lo]
        for n in range(10):
            ref = half if n in (1, 2, 5, 6, 7, 8) else whole
            rs_copy(c, n, ref, ref, other).wait_send()
        for h in range(4):
            att_copy(c, h).wait_send()

    block_of = {dest: b for b, dest in enumerate((RING[n % 4], n // 4) for n in range(8))}

    def out_products(c):
        for h in range(4):
            att_copy(c, h).wait_recv()
        events = {
            0: lambda: near_pair(c, 0),
            1: lambda: near_pair(c, 1),
            2: lambda: far_pair(c),
        }
        if c == 0:
            events[3] = lambda: near_free(c, 0)
            events[4] = lambda: near_free(c, 1)

        def one(i):
            b = pick(i, [block_of[dest] for dest in DESTS])
            term = None
            for owner in range(2):
                rows = jnp.concatenate([att[c, owner, h] for h in range(4)], axis=1)
                here = jnp.dot(rows, wo[owner, b], preferred_element_type=f32)
                term = here if term is None else term + here
            terms[c, i] = term.astype(bf16)
            for n, action in events.items():
                when(i, n, action)

        each(0, 8, one)

    def gather_event(n):
        if n == 2:
            g.from_sides(0)
        if n == 4:
            g.from_pair(0)
            g.pass_pair(0)
        if n == 5:
            g.from_far(0)
        if n == 6:
            g.pass_on(1)
            g.start_second(1)
            g.from_pair(1)
            g.pass_pair(1)
        if n == 7:
            g.from_last(0)
        if n == 8:
            g.from_pair_sides(0)
        if n == 11:
            kv.pass_on(0)
            g.from_sides(1)
        if n == 13:
            kv.from_sides(0)
            kv.from_pair(0)
            kv.pass_pair(0)
            kv.from_far(0)
            kv.from_pair_sides(0)
            g.from_last(1)

    def steps(first, last):
        def one(i):
            for n in (2, 4, 5, 6, 7, 8, 11, 13):
                if first <= n < last:
                    when(i, n, functools.partial(gather_event, n))
            code = pick(i - first, [c * 8 + b for c, b in PLAN[first:last]])
            c, b = code // 8, code % 8

            def ready():
                wq_copy(b).wait()
                wq_across(b).wait_recv()

            if any(c == 0 for c, b in PLAN[first:last]):
                pl.when(c == 0)(ready)
            project(c, b)

        each(first, last, one)

    g.pass_on(0)
    g.start_first(1)
    wk_copy.wait()
    wv_copy.wait()
    wk_across.wait_recv()
    wv_across.wait_recv()
    steps(0, 10)
    send_partials(0)
    partial_copy(0, 1).start()
    finish_kv(0)
    g.from_far(1)
    finish_q(0)
    steps(10, 14)
    kv.from_last(0)
    landed(0, 0, 4)
    g.from_pair_sides(1)
    late = [scaled_block(1, b) for b in (5, 6)]
    for b, (wide, scaled) in zip((5, 6), late):
        project_kv(1, b, wide, scaled)
    send_partials(1)
    for b, (wide, scaled) in zip((5, 6), late):
        project_q(1, b, scaled)
    partial_copy(1, 1).start()
    finish_kv(1)
    landed(0, 4, 8)
    finish_q(1)
    g.drain(0)
    g.drain(1)

    def near_keys():
        kv.from_sides(1)
        kv.from_pair(1)
        kv.pass_pair(1)

    unit(0, 0, 0, 8, True, False, (lambda: kv.pass_on(1), near_keys))
    kv.from_far(1)
    landed(1, 0, 4)
    unit(0, 1, 0, 4, False, False, (None, None, lambda: kv.from_pair_sides(1)))
    kv.from_last(1)
    landed(1, 4, 8)
    unit(0, 1, 4, 8, False, True)
    for b in range(8):
        wo_copy(b).wait()
        wo_across(b).wait_recv()
    out_products(0)
    unit(1, 0, 0, 8, True, False)
    unit(1, 1, 0, 4, False, False)
    unit(1, 1, 4, 8, False, True, (lambda: far_out(0),))
    out_products(1)
    here_in(0, 1)
    near_joined(0, 0)
    near_joined(0, 1)
    far_out(1)
    near_free(1, 0)
    near_free(1, 1)
    here_in(1, 1)
    here_in(0, 0)
    near_joined(1, 0)
    near_joined(1, 1)
    for b in range(8):
        wq_across(b).wait_send()
        wo_across(b).wait_send()
    wk_across.wait_send()
    wv_across.wait_send()
    for c in range(2):
        partial_copy(c, 0).wait_send()
        partial_copy(c, 1).wait_send()
        kv.drain(c)
    rs_drain(0)
    here_in(1, 0)
    rs_drain(1)


def hand_over(proj, norm, proj_out, norm_out):
    proj_out[...] = proj[...]
    norm_out[...] = norm[...]


def shards(
    checkpoint, norm_gain, query_weight, key_weight, value_weight, output_weight, block_order
):
    vmem = pl.BlockSpec(memory_space=pltpu.VMEM)
    hbm = pl.BlockSpec(memory_space=pl.ANY)
    dma = pltpu.SemaphoreType.DMA
    shapes = (
        jax.ShapeDtypeStruct((2 * ROWS, FEAT), bf16),
        jax.ShapeDtypeStruct((4, 2 * ROWS), f32),
    )
    results = pl.pallas_call(
        kernel,
        out_shape=shapes,
        in_specs=[pl.BlockSpec(memory_space=pltpu.SMEM), hbm, vmem, hbm, hbm, hbm, hbm],
        out_specs=(vmem, vmem),
        scratch_shapes=[
            pltpu.VMEM((2, 8, ROWS, FEAT), bf16),
            pltpu.VMEM((2, 8, FEAT, FEAT), bf16),
            pltpu.VMEM((2 * HEAD, D), bf16),
            pltpu.VMEM((2, 8, FEAT, FEAT), bf16),
            pltpu.VMEM((2, 2, ROWS, FEAT), f32),
            pltpu.VMEM((2, ROWS, 2 * HEAD), f32),
            pltpu.VMEM((2, ROWS, HEAD), f32),
            pltpu.VMEM((2, ROWS, 2 * HEAD), f32),
            pltpu.VMEM((2, ROWS, FEAT), f32),
            pltpu.VMEM((2, ROWS, 2 * HEAD), f32),
            pltpu.VMEM((2, ROWS, HEAD), f32),
            pltpu.VMEM((2, ROWS, HEAD), f32),
            pltpu.VMEM((2, 4, ROWS, HEAD), bf16),
            pltpu.VMEM((2, 2, N_CP, ROWS, HEAD), bf16),
            pltpu.VMEM((ROWS, N_CP * ROWS), f32),
            pltpu.VMEM((ROWS, N_CP * ROWS), f32),
            pltpu.VMEM((2, 4, ROWS, HEAD), f32),
            pltpu.VMEM((2, 4, ROWS, 2 * HEAD), f32),
            pltpu.VMEM((2, 2, 4, ROWS, HEAD), bf16),
            pltpu.VMEM((3, ROWS, ROWS), f32),
            pltpu.VMEM((2, 8, ROWS, FEAT), bf16),
            pltpu.VMEM((2, HALF, FEAT), bf16),
            pltpu.VMEM((2, HALF, FEAT), bf16),
            pltpu.VMEM((2, 2, ROWS, FEAT), bf16),
            pltpu.VMEM((2, 2, ROWS, FEAT), bf16),
            pltpu.VMEM((2, ROWS, FEAT), bf16),
            pltpu.VMEM((2, ROWS, FEAT), bf16),
            dma((2,)),
            dma((18,)),
            dma((22,)),
            dma((22,)),
            dma((20,)),
            dma((20,)),
            dma((36,)),
            dma((36,)),
            dma((8,)),
            dma((8,)),
            dma((20,)),
            dma((20,)),
        ],
        compiler_params=pltpu.CompilerParams(
            collective_id=0, has_side_effects=True, vmem_limit_bytes=63000000
        ),
        name="sublayer",
    )(
        block_order,
        checkpoint,
        norm_gain.reshape(D // HEAD, HEAD),
        query_weight,
        key_weight.T,
        value_weight.T,
        output_weight,
    )
    return pl.pallas_call(
        hand_over,
        out_shape=shapes,
        in_specs=[vmem, vmem],
        out_specs=(vmem, vmem),
        name="hand_over",
    )(*results)


def solution(mesh):
    return jax.shard_map(
        shards,
        mesh=mesh,
        in_specs=(
            P("cp", "tp"),
            P(),
            P(None, "tp"),
            P(None, "tp"),
            P(None, "tp"),
            P("tp", None),
            P(),
        ),
        out_specs=(P("cp", "tp"), P("tp", "cp")),
        check_vma=False,
    )
```

```python
import functools
import math

import jax
import jax.numpy as jnp
from jax import lax
from jax.experimental import pallas as pl
from jax.experimental.pallas import tpu as pltpu
from jax.sharding import PartitionSpec as P

MESH = pl.DeviceIdType.MESH
HEAD = 128
ROWS = 256
FEAT = 512
HALF = ROWS // 2
N_TP = 16
N_CP = 8
D = 8192
rope_base = 500000.0
norm_epsilon = 1e-05
masked_score = -1e30
LN2 = math.log(2.0)

f32 = jnp.float32
bf16 = jnp.bfloat16


def pick(i, values):
    out = values[-1]
    for n in range(len(values) - 2, -1, -1):
        out = jnp.where(i == n, values[n], out)
    return out


class Gather:
    def __init__(self, slot, ssem, rsem, right, left, pair, core=None):
        self.slot, self.ssem, self.rsem = slot, ssem, rsem
        self.right, self.left, self.pair, self.core = right, left, pair, core
        self.count = 10 if core is None else 18

    def ref(self, c, b, dk=0, rows=None):
        ref = self.slot(c, b, dk)
        return ref if rows is None else ref.at[pl.ds(rows * HALF, HALF)]

    def copy(self, c, n, ref, device):
        return pltpu.make_async_remote_copy(
            src_ref=ref,
            dst_ref=ref,
            send_sem=self.ssem.at[c * self.count + n],
            recv_sem=self.rsem.at[c * self.count + n],
            device_id=device,
            device_id_type=MESH,
        )

    def send_core(self, c, b):
        if self.core is not None:
            self.copy(c, 10 + b, self.ref(c, b), self.core).start()

    def start_pair(self, c):
        self.copy(c, 8, self.ref(c, 0), self.pair).start()
        self.send_core(c, 0)

    def start_first(self, c):
        self.copy(c, 0, self.ref(c, 0, rows=0), self.right).start()
        self.copy(c, 4, self.ref(c, 0, rows=1), self.left).start()

    def start_second(self, c):
        self.copy(c, 1, self.ref(c, 0, rows=1), self.right).start()
        self.copy(c, 5, self.ref(c, 0, rows=0), self.left).start()

    def pass_on(self, c):
        block = self.ref(c, 1, rows=0)
        self.copy(c, 0, block, self.left).wait_recv()
        self.copy(c, 2, block, self.right).start()
        block = self.ref(c, 2, rows=1)
        self.copy(c, 4, block, self.right).wait_recv()
        self.copy(c, 6, block, self.left).start()

    def from_sides(self, c):
        self.copy(c, 1, self.ref(c, 1, rows=1), self.left).wait_recv()
        self.send_core(c, 1)
        self.copy(c, 5, self.ref(c, 2, rows=0), self.right).wait_recv()
        self.send_core(c, 2)

    def from_pair(self, c):
        self.copy(c, 8, self.ref(c, 4), self.pair).wait_recv()
        self.send_core(c, 4)

    def pass_pair(self, c):
        block = self.ref(c, 4)
        self.copy(c, 3, block, self.right).start()
        self.copy(c, 7, block, self.left).start()

    def from_far(self, c):
        self.copy(c, 2, self.ref(c, 3, rows=0), self.left).wait_recv()
        self.copy(c, 6, self.ref(c, 3, rows=1), self.right).wait_recv()
        self.copy(c, 9, self.ref(c, 3), self.pair).start()
        self.send_core(c, 3)

    def from_pair_sides(self, c):
        self.copy(c, 3, self.ref(c, 5), self.left).wait_recv()
        self.send_core(c, 5)
        self.copy(c, 7, self.ref(c, 6), self.right).wait_recv()
        self.send_core(c, 6)

    def from_last(self, c):
        self.copy(c, 9, self.ref(c, 7), self.pair).wait_recv()
        self.send_core(c, 7)

    def from_core(self, c, b):
        self.copy(c, 10 + b, self.ref(c, b, dk=1), self.core).wait_recv()

    def drain(self, c):
        for n in range(self.count):
            ref = self.ref(c, 0, rows=0 if n in (0, 1, 2, 4, 5, 6) else None)
            self.copy(c, n, ref, self.pair).wait_send()


RING = (0, 3, 1, 2)
KEY_ORDER = (0, 1, 2, 4, 3, 5, 6, 7)
DESTS = ((1, 1), (3, 1), (2, 1), (1, 0), (3, 0), (2, 0), (0, 1), (0, 0))
PLAN = (
    (0, 0), (1, 0), (0, 1), (0, 2), (0, 4), (0, 3), (1, 4), (0, 7), (0, 5), (0, 6),
    (1, 3), (1, 1), (1, 2), (1, 7),
)


def kernel(
    order, x_hbm, gain, wq_hbm, wk_hbm, wv_hbm, wo_hbm,
    proj, norm_out,
    xg, wq, wkv, wo, acc_q, acc_kv, ss, part, part_q, part_kv, cos_t, sin_t, q, kvg,
    scr_a, scr_b, top, outs, att, bias, terms, ra, rb, rc, rd, re, ry,
    x_sem, w_sem, xs, xr, gs, gr, ks, kr, ps, pr, rs, rr,
):
    tp, cp = lax.axis_index("tp"), lax.axis_index("cp")
    core, yh, xx = tp % 2, (tp // 2) % 2, tp // 4
    yl, zz = cp % 2, cp // 2

    def tpi(dr, dp, dk):
        return (((xx + dr) % 4) * 2 + (yh + dp) % 2) * 2 + (core + dk) % 2

    def cpi(dr, dp):
        return ((zz + dr) % 4) * 2 + (yl + dp) % 2

    right, left = {"tp": tpi(1, 0, 0)}, {"tp": tpi(3, 0, 0)}
    pair, other = {"tp": tpi(0, 1, 0)}, {"tp": tpi(0, 0, 1)}
    up, down, beside = {"cp": cpi(1, 0)}, {"cp": cpi(3, 0)}, {"cp": cpi(0, 1)}

    def chip(b):
        dr = RING[b % 4] if isinstance(b, int) else pick(b % 4, RING)
        return ((xx + dr) % 4) * 2 + (yh + b // 4) % 2

    def tp_slot(b, dk):
        return chip(b) * 2 + (core + dk) % 2

    def kv_slot(b):
        dr = RING[b % 4] if isinstance(b, int) else pick(b % 4, RING)
        return cpi(dr, b // 4)

    x_copies = [
        pltpu.make_async_copy(x_hbm.at[pl.ds(c * ROWS, ROWS)], xg.at[c, tp // 2], x_sem.at[c])
        for c in range(2)
    ]
    for copy in x_copies:
        copy.start()

    def features(b, dk):
        return pl.ds(pl.multiple_of(tp_slot(b, dk) * FEAT, FEAT), FEAT)

    def to_other(n, src, dst):
        return pltpu.make_async_remote_copy(
            src_ref=src,
            dst_ref=dst,
            send_sem=xs.at[n],
            recv_sem=xr.at[n],
            device_id=other,
            device_id_type=MESH,
        )

    def wq_copy(b):
        return pltpu.make_async_copy(wq_hbm.at[features(b, 0)], wq.at[0, b], w_sem.at[b])

    def wo_copy(b):
        return pltpu.make_async_copy(wo_hbm.at[:, features(b, 0)], wo.at[0, b], w_sem.at[8 + b])

    def wq_across(b):
        return to_other(b, wq_hbm.at[features(b, 1)], wq.at[1, b])

    def wo_across(b):
        return to_other(8 + b, wo_hbm.at[:, features(b, 1)], wo.at[1, b])

    outer = pl.ds(pl.multiple_of(192 * core, 64), 64)
    inner = pl.ds(pl.multiple_of(128 - 64 * core, 64), 64)
    wk_copy = pltpu.make_async_copy(wk_hbm, wkv.at[outer], w_sem.at[16])
    wv_copy = pltpu.make_async_copy(wv_hbm, wkv.at[inner], w_sem.at[17])
    wk_across = to_other(16, wk_hbm, wkv.at[inner])
    wv_across = to_other(17, wv_hbm, wkv.at[outer])

    barrier = pltpu.get_barrier_semaphore()
    neighbours = (right, left, pair, other, up, down, beside)
    for device in neighbours:
        pl.semaphore_signal(barrier, inc=1, device_id=device, device_id_type=MESH)

    first_use = (0, 1, 2, 4, 3, 7, 5, 6)
    wk_copy.start()
    wv_copy.start()
    for b in first_use:
        wq_copy(b).start()
    for b in range(8):
        wo_copy(b).start()

    pl.semaphore_wait(barrier, len(neighbours))

    g = Gather(lambda c, b, dk: xg.at[c, chip(b)], gs, gr, right, left, pair)
    kv = Gather(
        lambda c, b, dk: kvg.at[c, (core + dk) % 2, kv_slot(b)], ks, kr, up, down, beside, other
    )

    x_copies[0].wait()
    g.start_pair(0)
    g.start_first(0)
    g.start_second(0)
    x_copies[1].wait()
    g.start_pair(1)
    wk_across.start()
    wv_across.start()
    for b in first_use:
        wq_across(b).start()
    for b in range(8):
        wo_across(b).start()

    row_id = lax.broadcasted_iota(jnp.int32, (ROWS, ROWS), 0)
    col_id = lax.broadcasted_iota(jnp.int32, (ROWS, ROWS), 1)
    bias[0] = jnp.zeros((ROWS, ROWS), f32)
    bias[1] = jnp.where(col_id <= row_id, 0.0, masked_score).astype(f32)
    bias[2] = jnp.full((ROWS, ROWS), masked_score, f32)
    acc_q[...] = jnp.zeros_like(acc_q)
    acc_kv[...] = jnp.zeros_like(acc_kv)
    ss[...] = jnp.zeros_like(ss)

    even = (lax.broadcasted_iota(jnp.int32, (ROWS, HEAD), 1) % 2) == 0

    def make_tables():
        lane8 = lax.broadcasted_iota(jnp.int32, (8, HEAD), 1)
        rate8 = jnp.exp2((lane8 // 2).astype(f32) * (-2.0 / HEAD * math.log2(rope_base)))
        rate = jnp.broadcast_to(rate8[:1], (ROWS, HEAD))
        angle = lax.broadcasted_iota(jnp.int32, (ROWS, HEAD), 0).astype(f32) * rate
        cos_r, sin_r = jnp.cos(angle), jnp.sin(angle)
        sign = jnp.where(even, -1.0, 1.0).astype(f32)
        for c in range(2):
            start = (order[2 * cp + c] * ROWS).astype(f32) * rate8
            cos_b, sin_b = jnp.cos(start)[:1], jnp.sin(start)[:1]
            cos_t[c] = cos_b * cos_r - sin_b * sin_r
            sin_t[c] = (sin_b * cos_r + cos_b * sin_r) * sign

    make_tables()

    def scaled_block(c, b):
        wide = xg[c, chip(b)].astype(f32)
        j = tp_slot(b, 0)
        pieces = [
            (wide[:, n * HEAD : (n + 1) * HEAD] * gain[pl.ds(4 * j + n, 1), :]).astype(bf16)
            for n in range(4)
        ]
        return wide, jnp.concatenate(pieces, axis=1)

    def project_kv(c, b, wide, scaled):
        square = wide * wide
        ss[c] += square[:, :128] + square[:, 128:256] + square[:, 256:384] + square[:, 384:]
        acc_kv[c] += lax.dot_general(
            scaled, wkv[:, features(b, 0)], (((1,), (1,)), ((), ())), preferred_element_type=f32
        )

    def project_q(c, b, scaled):
        for owner in range(2):
            acc_q[c, owner] += jnp.dot(scaled, wq[owner, b], preferred_element_type=f32)

    def project(c, b):
        wide, scaled = scaled_block(c, b)
        project_kv(c, b, wide, scaled)
        project_q(c, b, scaled)

    def partial_copy(c, n):
        if n == 0:
            return to_other(18 + c, part.at[c], part_kv.at[c])
        return to_other(20 + c, acc_q.at[c, 1], part_q.at[c])

    def send_partials(c):
        part[c, :, :HEAD] = acc_kv[c, :, HEAD:]
        part[c, :, HEAD:] = ss[c]
        partial_copy(c, 0).start()

    def turn(y, cosine, sine):
        swapped = jnp.where(even, pltpu.roll(y, HEAD - 1, 1), pltpu.roll(y, 1, 1))
        return y * cosine + swapped * sine

    def finish_kv(c):
        partial_copy(c, 0).wait_recv()
        squares = jnp.sum(ss[c] + part_kv[c, :, HEAD:], axis=1, keepdims=True)
        scale = jnp.broadcast_to(lax.rsqrt(squares * (1.0 / D) + norm_epsilon), (ROWS, HEAD))
        ss[c] = scale
        cosine, sine = cos_t[c], sin_t[c]
        both = (acc_kv[c, :, :HEAD] + part_kv[c, :, :HEAD]) * scale
        turned = turn(both, cosine, sine)
        keys = jnp.concatenate([turned[:HALF].T, turned[HALF:].T], axis=0)
        kvg[c, core, cp] = jnp.where(core == 0, keys, both).astype(bf16)
        kv.start_pair(c)
        kv.start_first(c)
        kv.start_second(c)

    def finish_q(c):
        partial_copy(c, 1).wait_recv()
        cosine, sine = cos_t[c], sin_t[c]
        q_scale = ss[c] * (math.log2(math.e) / math.sqrt(HEAD))
        for h in range(4):
            lanes = slice(h * HEAD, (h + 1) * HEAD)
            y = (acc_q[c, 0, :, lanes] + part_q[c, :, lanes]) * q_scale
            q[c, h] = turn(y, cosine, sine).astype(bf16)

    def each(first, last, body):
        def one(i, unused):
            body(i)
            return unused

        lax.fori_loop(first, last, one, 0)

    def when(i, n, action):
        pl.when(i == n)(action)

    def landed(c, first, last):
        for b in KEY_ORDER[first:last]:
            kv.from_core(c, b)

    def unit(qc, kc, start, stop, first, last, between=()):
        q_block = order[2 * cp + qc]
        which, slots = {}, {}
        for p in range(start, stop):
            slots[p] = kv_slot(KEY_ORDER[p])
            k_block = order[2 * slots[p] + kc]
            which[p] = jnp.where(k_block < q_block, 0, jnp.where(k_block == q_block, 1, 2))
        group = 4
        tops = {}

        def score(h, p, best):
            scr = (scr_a, scr_b)[h % 2]
            halves = [kvg[kc, 0, slots[p], :HALF], kvg[kc, 0, slots[p], HALF:]]
            keys = jnp.concatenate(halves, axis=1)
            scores = jnp.dot(q[qc, h], keys, preferred_element_type=f32) + bias[which[p]]
            scr[:, p * ROWS : (p + 1) * ROWS] = scores
            here = jnp.maximum(scores[:, :HEAD], scores[:, HEAD:])
            return here if best is None else jnp.maximum(best, here)

        def settle(h, best):
            new_top = jnp.broadcast_to(jnp.max(best, axis=1, keepdims=True), (ROWS, HEAD))
            tops[h] = new_top if first else jnp.maximum(top[qc, h], new_top)

        def weigh(h, p, total):
            scr = (scr_a, scr_b)[h % 2]
            both = jnp.concatenate([tops[h]] * 2, axis=1)
            weights = [
                jnp.exp2(scr[:, n * ROWS : (n + 1) * ROWS] - both).astype(bf16)
                for n in range(p, p + group)
            ]
            values = jnp.concatenate([kvg[kc, 1, slots[n]] for n in range(p, p + group)], axis=0)
            here = jnp.dot(
                jnp.concatenate(weights, axis=1),
                jnp.concatenate([values, jnp.ones((group * ROWS, HEAD), bf16)], axis=1),
                preferred_element_type=f32,
            )
            return here if total is None else total + here

        def close(h, total):
            if not first:
                shrink = jnp.exp2(top[qc, h] - tops[h])
                total = total + outs[qc, h] * jnp.concatenate([shrink, shrink], axis=1)
            if last:
                sums = total[:, HEAD:]
                att[qc, 0, h] = (total[:, :HEAD] / sums).astype(bf16)
                att_copy(qc, h).start()
                normalizer = (tops[h] + jnp.log2(sums)) * LN2
                norm_out[h : h + 1, qc * ROWS : (qc + 1) * ROWS] = normalizer.T[:1]
            else:
                top[qc, h] = tops[h]
                outs[qc, h] = total

        best = None
        for p in range(start, stop):
            best = score(0, p, best)
        settle(0, best)
        for h in range(4):
            best = total = None
            for p in range(start, stop):
                if h < 3:
                    best = score(h + 1, p, best)
                if p % group == group - 1:
                    total = weigh(h, p - group + 1, total)
            close(h, total)
            if h < 3:
                settle(h + 1, best)
            if h < len(between) and between[h] is not None:
                between[h]()

    def att_copy(c, h):
        return pltpu.make_async_remote_copy(
            src_ref=att.at[c, 0, h],
            dst_ref=att.at[c, 1, h],
            send_sem=ps.at[c * 4 + h],
            recv_sem=pr.at[c * 4 + h],
            device_id=other,
            device_id_type=MESH,
        )

    def rs_copy(c, n, src, dst, device):
        return pltpu.make_async_remote_copy(
            src_ref=src,
            dst_ref=dst,
            send_sem=rs.at[c * 10 + n],
            recv_sem=rr.at[c * 10 + n],
            device_id=device,
            device_id_type=MESH,
        )

    lo, hi = pl.ds(0, HALF), pl.ds(HALF, HALF)
    ways = (right, left)

    def far_pair(c):
        rs_copy(c, 0, terms.at[c, 2], re.at[c], pair).start()

    def far_out(c):
        block = terms.at[c, 5]
        rs_copy(c, 0, re.at[c], re.at[c], pair).wait_recv()
        block[...] = (block[...].astype(f32) + re[c].astype(f32)).astype(bf16)
        rs_copy(c, 1, block.at[lo], ra.at[c], right).start()
        rs_copy(c, 2, block.at[hi], rb.at[c], left).start()

    def near_pair(c, side):
        rs_copy(c, 3 + side, terms.at[c, side], (rc, rd)[side].at[c, 1], ways[side]).start()

    def near_free(c, side):
        half = (hi, lo)[side]
        rs_copy(
            c, 5 + side, terms.at[c, 3 + side].at[half], (rc, rd)[side].at[c, 0].at[half], ways[side]
        ).start()

    def near_joined(c, side):
        half = (lo, hi)[side]
        block, moved = terms.at[c, 3 + side].at[half], (ra, rb)[side].at[c]
        rs_copy(c, 1 + side, moved, moved, left).wait_recv()
        block[...] = (block[...].astype(f32) + moved[...].astype(f32)).astype(bf16)
        rs_copy(c, 7 + side, block, (rc, rd)[side].at[c, 0].at[half], ways[side]).start()

    def here_in(c, p):
        term = terms[c, 7 - p].astype(f32)
        for side in range(2):
            block = (rc, rd)[side].at[c, p]
            if p == 1:
                rs_copy(c, 3 + side, block, block, left).wait_recv()
            else:
                for n, half in ((5, (hi, lo)[side]), (7, (lo, hi)[side])):
                    rs_copy(c, n + side, block.at[half], block.at[half], left).wait_recv()
            term = term + block[...].astype(f32)
        if p == 1:
            block = terms.at[c, 6]
            block[...] = term.astype(bf16)
            rs_copy(c, 9, block, ry.at[c], pair).start()
        else:
            rs_copy(c, 9, ry.at[c], ry.at[c], pair).wait_recv()
            proj[c * ROWS : (c + 1) * ROWS] = (term + ry[c].astype(f32)).astype(bf16)

    def rs_drain(c):
        whole, half = terms.at[c, 0], terms.at[c, 0, lo]
        for n in range(10):
            ref = half if n in (1, 2, 5, 6, 7, 8) else whole
            rs_copy(c, n, ref, ref, other).wait_send()
        for h in range(4):
            att_copy(c, h).wait_send()

    block_of = {dest: b for b, dest in enumerate((RING[n % 4], n // 4) for n in range(8))}

    def out_products(c):
        for h in range(4):
            att_copy(c, h).wait_recv()
        events = {
            0: lambda: near_pair(c, 0),
            1: lambda: near_pair(c, 1),
            2: lambda: far_pair(c),
        }
        if c == 0:
            events[3] = lambda: near_free(c, 0)
            events[4] = lambda: near_free(c, 1)

        def one(i):
            b = pick(i, [block_of[dest] for dest in DESTS])
            term = None
            for owner in range(2):
                rows = jnp.concatenate([att[c, owner, h] for h in range(4)], axis=1)
                here = jnp.dot(rows, wo[owner, b], preferred_element_type=f32)
                term = here if term is None else term + here
            terms[c, i] = term.astype(bf16)
            for n, action in events.items():
                when(i, n, action)

        each(0, 8, one)

    def gather_event(n):
        if n == 2:
            g.from_sides(0)
        if n == 4:
            g.from_pair(0)
            g.pass_pair(0)
        if n == 5:
            g.from_far(0)
        if n == 6:
            g.pass_on(1)
            g.start_second(1)
            g.from_pair(1)
            g.pass_pair(1)
        if n == 7:
            g.from_last(0)
        if n == 8:
            g.from_pair_sides(0)
        if n == 11:
            kv.pass_on(0)
            g.from_sides(1)
        if n == 13:
            kv.from_sides(0)
            kv.from_pair(0)
            kv.pass_pair(0)
            kv.from_far(0)
            kv.from_pair_sides(0)
            g.from_last(1)

    def steps(first, last):
        def one(i):
            for n in (2, 4, 5, 6, 7, 8, 11, 13):
                if first <= n < last:
                    when(i, n, functools.partial(gather_event, n))
            code = pick(i - first, [c * 8 + b for c, b in PLAN[first:last]])
            c, b = code // 8, code % 8

            def ready():
                wq_copy(b).wait()
                wq_across(b).wait_recv()

            if any(c == 0 for c, b in PLAN[first:last]):
                pl.when(c == 0)(ready)
            project(c, b)

        each(first, last, one)

    g.pass_on(0)
    g.start_first(1)
    wk_copy.wait()
    wv_copy.wait()
    wk_across.wait_recv()
    wv_across.wait_recv()
    steps(0, 10)
    send_partials(0)
    partial_copy(0, 1).start()
    finish_kv(0)
    g.from_far(1)
    finish_q(0)
    steps(10, 14)
    kv.from_last(0)
    landed(0, 0, 4)
    g.from_pair_sides(1)
    late = [scaled_block(1, b) for b in (5, 6)]
    for b, (wide, scaled) in zip((5, 6), late):
        project_kv(1, b, wide, scaled)
    send_partials(1)
    for b, (wide, scaled) in zip((5, 6), late):
        project_q(1, b, scaled)
    partial_copy(1, 1).start()
    finish_kv(1)
    landed(0, 4, 8)
    finish_q(1)
    g.drain(0)
    g.drain(1)

    def near_keys():
        kv.from_sides(1)
        kv.from_pair(1)
        kv.pass_pair(1)

    unit(0, 0, 0, 8, True, False, (lambda: kv.pass_on(1), near_keys))
    kv.from_far(1)
    landed(1, 0, 4)
    unit(0, 1, 0, 4, False, False, (None, None, lambda: kv.from_pair_sides(1)))
    kv.from_last(1)
    landed(1, 4, 8)
    unit(0, 1, 4, 8, False, True)
    for b in range(8):
        wo_copy(b).wait()
        wo_across(b).wait_recv()
    out_products(0)
    unit(1, 0, 0, 8, True, False)
    unit(1, 1, 0, 4, False, False)
    unit(1, 1, 4, 8, False, True, (lambda: far_out(0),))
    out_products(1)
    here_in(0, 1)
    near_joined(0, 0)
    near_joined(0, 1)
    far_out(1)
    near_free(1, 0)
    near_free(1, 1)
    here_in(1, 1)
    here_in(0, 0)
    near_joined(1, 0)
    near_joined(1, 1)
    for b in range(8):
        wq_across(b).wait_send()
        wo_across(b).wait_send()
    wk_across.wait_send()
    wv_across.wait_send()
    for c in range(2):
        partial_copy(c, 0).wait_send()
        partial_copy(c, 1).wait_send()
        kv.drain(c)
    rs_drain(0)
    here_in(1, 0)
    rs_drain(1)


def hand_over(proj, norm, proj_out, norm_out):
    proj_out[...] = proj[...]
    norm_out[...] = norm[...]


def shards(
    checkpoint, norm_gain, query_weight, key_weight, value_weight, output_weight, block_order
):
    vmem = pl.BlockSpec(memory_space=pltpu.VMEM)
    hbm = pl.BlockSpec(memory_space=pl.ANY)
    dma = pltpu.SemaphoreType.DMA
    shapes = (
        jax.ShapeDtypeStruct((2 * ROWS, FEAT), bf16),
        jax.ShapeDtypeStruct((4, 2 * ROWS), f32),
    )
    results = pl.pallas_call(
        kernel,
        out_shape=tuple(pltpu.VMEM(shape.shape, shape.dtype) for shape in shapes),
        in_specs=[pl.BlockSpec(memory_space=pltpu.SMEM), hbm, vmem, hbm, hbm, hbm, hbm],
        out_specs=(vmem, vmem),
        scratch_shapes=[
            pltpu.VMEM((2, 8, ROWS, FEAT), bf16),
            pltpu.VMEM((2, 8, FEAT, FEAT), bf16),
            pltpu.VMEM((2 * HEAD, D), bf16),
            pltpu.VMEM((2, 8, FEAT, FEAT), bf16),
            pltpu.VMEM((2, 2, ROWS, FEAT), f32),
            pltpu.VMEM((2, ROWS, 2 * HEAD), f32),
            pltpu.VMEM((2, ROWS, HEAD), f32),
            pltpu.VMEM((2, ROWS, 2 * HEAD), f32),
            pltpu.VMEM((2, ROWS, FEAT), f32),
            pltpu.VMEM((2, ROWS, 2 * HEAD), f32),
            pltpu.VMEM((2, ROWS, HEAD), f32),
            pltpu.VMEM((2, ROWS, HEAD), f32),
            pltpu.VMEM((2, 4, ROWS, HEAD), bf16),
            pltpu.VMEM((2, 2, N_CP, ROWS, HEAD), bf16),
            pltpu.VMEM((ROWS, N_CP * ROWS), f32),
            pltpu.VMEM((ROWS, N_CP * ROWS), f32),
            pltpu.VMEM((2, 4, ROWS, HEAD), f32),
            pltpu.VMEM((2, 4, ROWS, 2 * HEAD), f32),
            pltpu.VMEM((2, 2, 4, ROWS, HEAD), bf16),
            pltpu.VMEM((3, ROWS, ROWS), f32),
            pltpu.VMEM((2, 8, ROWS, FEAT), bf16),
            pltpu.VMEM((2, HALF, FEAT), bf16),
            pltpu.VMEM((2, HALF, FEAT), bf16),
            pltpu.VMEM((2, 2, ROWS, FEAT), bf16),
            pltpu.VMEM((2, 2, ROWS, FEAT), bf16),
            pltpu.VMEM((2, ROWS, FEAT), bf16),
            pltpu.VMEM((2, ROWS, FEAT), bf16),
            dma((2,)),
            dma((18,)),
            dma((22,)),
            dma((22,)),
            dma((20,)),
            dma((20,)),
            dma((36,)),
            dma((36,)),
            dma((8,)),
            dma((8,)),
            dma((20,)),
            dma((20,)),
        ],
        compiler_params=pltpu.CompilerParams(
            collective_id=0, has_side_effects=True, vmem_limit_bytes=63000000
        ),
        name="sublayer",
    )(
        block_order,
        checkpoint,
        norm_gain.reshape(D // HEAD, HEAD),
        query_weight,
        key_weight.T,
        value_weight.T,
        output_weight,
    )
    return pl.pallas_call(
        hand_over,
        out_shape=shapes,
        in_specs=[vmem, vmem],
        out_specs=(vmem, vmem),
        name="hand_over",
    )(*(pltpu.with_memory_space_constraint(result, pltpu.VMEM) for result in results))


def solution(mesh):
    return jax.shard_map(
        shards,
        mesh=mesh,
        in_specs=(
            P("cp", "tp"),
            P(),
            P(None, "tp"),
            P(None, "tp"),
            P(None, "tp"),
            P("tp", None),
            P(),
        ),
        out_specs=(P("cp", "tp"), P("tp", "cp")),
        check_vma=False,
    )
```

```python
import functools
import math

import jax
import jax.numpy as jnp
from jax import lax
from jax.experimental import pallas as pl
from jax.experimental.pallas import tpu as pltpu
from jax.sharding import PartitionSpec as P

MESH = pl.DeviceIdType.MESH
HEAD = 128
ROWS = 256
FEAT = 512
HALF = ROWS // 2
N_TP = 16
N_CP = 8
D = 8192
rope_base = 500000.0
norm_epsilon = 1e-05
masked_score = -1e30
LN2 = math.log(2.0)

f32 = jnp.float32
bf16 = jnp.bfloat16


def pick(i, values):
    out = values[-1]
    for n in range(len(values) - 2, -1, -1):
        out = jnp.where(i == n, values[n], out)
    return out


class Gather:
    def __init__(self, slot, ssem, rsem, right, left, pair, core=None):
        self.slot, self.ssem, self.rsem = slot, ssem, rsem
        self.right, self.left, self.pair, self.core = right, left, pair, core
        self.count = 10 if core is None else 18

    def ref(self, c, b, dk=0, rows=None):
        ref = self.slot(c, b, dk)
        return ref if rows is None else ref.at[pl.ds(rows * HALF, HALF)]

    def copy(self, c, n, ref, device):
        return pltpu.make_async_remote_copy(
            src_ref=ref,
            dst_ref=ref,
            send_sem=self.ssem.at[c * self.count + n],
            recv_sem=self.rsem.at[c * self.count + n],
            device_id=device,
            device_id_type=MESH,
        )

    def send_core(self, c, b):
        if self.core is not None:
            self.copy(c, 10 + b, self.ref(c, b), self.core).start()

    def start_pair(self, c):
        self.copy(c, 8, self.ref(c, 0), self.pair).start()
        self.send_core(c, 0)

    def start_first(self, c):
        self.copy(c, 0, self.ref(c, 0, rows=0), self.right).start()
        self.copy(c, 4, self.ref(c, 0, rows=1), self.left).start()

    def start_second(self, c):
        self.copy(c, 1, self.ref(c, 0, rows=1), self.right).start()
        self.copy(c, 5, self.ref(c, 0, rows=0), self.left).start()

    def pass_on(self, c):
        block = self.ref(c, 1, rows=0)
        self.copy(c, 0, block, self.left).wait_recv()
        self.copy(c, 2, block, self.right).start()
        block = self.ref(c, 2, rows=1)
        self.copy(c, 4, block, self.right).wait_recv()
        self.copy(c, 6, block, self.left).start()

    def from_sides(self, c):
        self.copy(c, 1, self.ref(c, 1, rows=1), self.left).wait_recv()
        self.send_core(c, 1)
        self.copy(c, 5, self.ref(c, 2, rows=0), self.right).wait_recv()
        self.send_core(c, 2)

    def from_pair(self, c):
        self.copy(c, 8, self.ref(c, 4), self.pair).wait_recv()
        self.send_core(c, 4)

    def pass_pair(self, c):
        block = self.ref(c, 4)
        self.copy(c, 3, block, self.right).start()
        self.copy(c, 7, block, self.left).start()

    def from_far(self, c):
        self.copy(c, 2, self.ref(c, 3, rows=0), self.left).wait_recv()
        self.copy(c, 6, self.ref(c, 3, rows=1), self.right).wait_recv()
        self.copy(c, 9, self.ref(c, 3), self.pair).start()
        self.send_core(c, 3)

    def from_pair_sides(self, c):
        self.copy(c, 3, self.ref(c, 5), self.left).wait_recv()
        self.send_core(c, 5)
        self.copy(c, 7, self.ref(c, 6), self.right).wait_recv()
        self.send_core(c, 6)

    def from_last(self, c):
        self.copy(c, 9, self.ref(c, 7), self.pair).wait_recv()
        self.send_core(c, 7)

    def from_core(self, c, b):
        self.copy(c, 10 + b, self.ref(c, b, dk=1), self.core).wait_recv()

    def drain(self, c):
        for n in range(self.count):
            ref = self.ref(c, 0, rows=0 if n in (0, 1, 2, 4, 5, 6) else None)
            self.copy(c, n, ref, self.pair).wait_send()


RING = (0, 3, 1, 2)
KEY_ORDER = (0, 1, 2, 4, 3, 5, 6, 7)
DESTS = ((1, 1), (3, 1), (2, 1), (1, 0), (3, 0), (2, 0), (0, 1), (0, 0))
PLAN = (
    (0, 0), (1, 0), (0, 1), (0, 2), (0, 4), (0, 3), (1, 4), (0, 7), (0, 5), (0, 6),
    (1, 3), (1, 1), (1, 2), (1, 7),
)


def kernel(
    order, x_hbm, gain, wq_hbm, wk_hbm, wv_hbm, wo_hbm,
    proj, norm_out,
    xg, wq, wkv, wo, acc_q, acc_kv, ss, part, part_q, part_kv, cos_t, sin_t, q, kvg,
    scr_a, scr_b, top, outs, att, bias, terms, ra, rb, rc, rd, re, ry,
    x_sem, w_sem, xs, xr, gs, gr, ks, kr, ps, pr, rs, rr,
):
    tp, cp = lax.axis_index("tp"), lax.axis_index("cp")
    core, yh, xx = tp % 2, (tp // 2) % 2, tp // 4
    yl, zz = cp % 2, cp // 2

    def tpi(dr, dp, dk):
        return (((xx + dr) % 4) * 2 + (yh + dp) % 2) * 2 + (core + dk) % 2

    def cpi(dr, dp):
        return ((zz + dr) % 4) * 2 + (yl + dp) % 2

    right, left = {"tp": tpi(1, 0, 0)}, {"tp": tpi(3, 0, 0)}
    pair, other = {"tp": tpi(0, 1, 0)}, {"tp": tpi(0, 0, 1)}
    up, down, beside = {"cp": cpi(1, 0)}, {"cp": cpi(3, 0)}, {"cp": cpi(0, 1)}

    def chip(b):
        dr = RING[b % 4] if isinstance(b, int) else pick(b % 4, RING)
        return ((xx + dr) % 4) * 2 + (yh + b // 4) % 2

    def tp_slot(b, dk):
        return chip(b) * 2 + (core + dk) % 2

    def kv_slot(b):
        dr = RING[b % 4] if isinstance(b, int) else pick(b % 4, RING)
        return cpi(dr, b // 4)

    x_copies = [
        pltpu.make_async_copy(x_hbm.at[pl.ds(c * ROWS, ROWS)], xg.at[c, tp // 2], x_sem.at[c])
        for c in range(2)
    ]
    for copy in x_copies:
        copy.start()

    def features(b, dk):
        return pl.ds(pl.multiple_of(tp_slot(b, dk) * FEAT, FEAT), FEAT)

    def to_other(n, src, dst):
        return pltpu.make_async_remote_copy(
            src_ref=src,
            dst_ref=dst,
            send_sem=xs.at[n],
            recv_sem=xr.at[n],
            device_id=other,
            device_id_type=MESH,
        )

    def wq_copy(b):
        return pltpu.make_async_copy(wq_hbm.at[features(b, 0)], wq.at[0, b], w_sem.at[b])

    def wo_copy(b):
        return pltpu.make_async_copy(wo_hbm.at[:, features(b, 0)], wo.at[0, b], w_sem.at[8 + b])

    def wq_across(b):
        return to_other(b, wq_hbm.at[features(b, 1)], wq.at[1, b])

    def wo_across(b):
        return to_other(8 + b, wo_hbm.at[:, features(b, 1)], wo.at[1, b])

    outer = pl.ds(pl.multiple_of(192 * core, 64), 64)
    inner = pl.ds(pl.multiple_of(128 - 64 * core, 64), 64)
    wk_copy = pltpu.make_async_copy(wk_hbm, wkv.at[outer], w_sem.at[16])
    wv_copy = pltpu.make_async_copy(wv_hbm, wkv.at[inner], w_sem.at[17])
    wk_across = to_other(16, wk_hbm, wkv.at[inner])
    wv_across = to_other(17, wv_hbm, wkv.at[outer])

    barrier = pltpu.get_barrier_semaphore()
    neighbours = (right, left, pair, other, up, down, beside)
    for device in neighbours:
        pl.semaphore_signal(barrier, inc=1, device_id=device, device_id_type=MESH)

    first_use = (0, 1, 2, 4, 3, 7, 5, 6)
    wk_copy.start()
    wv_copy.start()
    for b in first_use:
        wq_copy(b).start()
    for b in range(8):
        wo_copy(b).start()

    pl.semaphore_wait(barrier, len(neighbours))

    g = Gather(lambda c, b, dk: xg.at[c, chip(b)], gs, gr, right, left, pair)
    kv = Gather(
        lambda c, b, dk: kvg.at[c, (core + dk) % 2, kv_slot(b)], ks, kr, up, down, beside, other
    )

    x_copies[0].wait()
    g.start_pair(0)
    g.start_first(0)
    g.start_second(0)
    x_copies[1].wait()
    g.start_pair(1)
    wk_across.start()
    wv_across.start()
    for b in first_use:
        wq_across(b).start()
    for b in range(8):
        wo_across(b).start()

    row_id = lax.broadcasted_iota(jnp.int32, (ROWS, ROWS), 0)
    col_id = lax.broadcasted_iota(jnp.int32, (ROWS, ROWS), 1)
    bias[0] = jnp.zeros((ROWS, ROWS), f32)
    bias[1] = jnp.where(col_id <= row_id, 0.0, masked_score).astype(f32)
    bias[2] = jnp.full((ROWS, ROWS), masked_score, f32)
    acc_q[...] = jnp.zeros_like(acc_q)
    acc_kv[...] = jnp.zeros_like(acc_kv)
    ss[...] = jnp.zeros_like(ss)

    even = (lax.broadcasted_iota(jnp.int32, (ROWS, HEAD), 1) % 2) == 0

    def make_tables():
        lane8 = lax.broadcasted_iota(jnp.int32, (8, HEAD), 1)
        rate8 = jnp.exp2((lane8 // 2).astype(f32) * (-2.0 / HEAD * math.log2(rope_base)))
        rate = jnp.broadcast_to(rate8[:1], (ROWS, HEAD))
        angle = lax.broadcasted_iota(jnp.int32, (ROWS, HEAD), 0).astype(f32) * rate
        cos_r, sin_r = jnp.cos(angle), jnp.sin(angle)
        sign = jnp.where(even, -1.0, 1.0).astype(f32)
        for c in range(2):
            start = (order[2 * cp + c] * ROWS).astype(f32) * rate8
            cos_b, sin_b = jnp.cos(start)[:1], jnp.sin(start)[:1]
            cos_t[c] = cos_b * cos_r - sin_b * sin_r
            sin_t[c] = (sin_b * cos_r + cos_b * sin_r) * sign

    make_tables()

    def scaled_block(c, b):
        wide = xg[c, chip(b)].astype(f32)
        j = tp_slot(b, 0)
        pieces = [
            (wide[:, n * HEAD : (n + 1) * HEAD] * gain[pl.ds(4 * j + n, 1), :]).astype(bf16)
            for n in range(4)
        ]
        return wide, jnp.concatenate(pieces, axis=1)

    def project_kv(c, b, wide, scaled):
        square = wide * wide
        ss[c] += square[:, :128] + square[:, 128:256] + square[:, 256:384] + square[:, 384:]
        acc_kv[c] += lax.dot_general(
            scaled, wkv[:, features(b, 0)], (((1,), (1,)), ((), ())), preferred_element_type=f32
        )

    def project_q(c, b, scaled):
        for owner in range(2):
            acc_q[c, owner] += jnp.dot(scaled, wq[owner, b], preferred_element_type=f32)

    def project(c, b):
        wide, scaled = scaled_block(c, b)
        project_kv(c, b, wide, scaled)
        project_q(c, b, scaled)

    def partial_copy(c, n):
        if n == 0:
            return to_other(18 + c, part.at[c], part_kv.at[c])
        return to_other(20 + c, acc_q.at[c, 1], part_q.at[c])

    def send_partials(c):
        part[c, :, :HEAD] = acc_kv[c, :, HEAD:]
        part[c, :, HEAD:] = ss[c]
        partial_copy(c, 0).start()

    def turn(y, cosine, sine):
        swapped = jnp.where(even, pltpu.roll(y, HEAD - 1, 1), pltpu.roll(y, 1, 1))
        return y * cosine + swapped * sine

    def finish_kv(c):
        partial_copy(c, 0).wait_recv()
        squares = jnp.sum(ss[c] + part_kv[c, :, HEAD:], axis=1, keepdims=True)
        scale = jnp.broadcast_to(lax.rsqrt(squares * (1.0 / D) + norm_epsilon), (ROWS, HEAD))
        ss[c] = scale
        cosine, sine = cos_t[c], sin_t[c]
        both = (acc_kv[c, :, :HEAD] + part_kv[c, :, :HEAD]) * scale
        turned = turn(both, cosine, sine)
        keys = jnp.concatenate([turned[:HALF].T, turned[HALF:].T], axis=0)
        kvg[c, core, cp] = jnp.where(core == 0, keys, both).astype(bf16)
        kv.start_pair(c)
        kv.start_first(c)
        kv.start_second(c)

    def finish_q(c):
        partial_copy(c, 1).wait_recv()
        cosine, sine = cos_t[c], sin_t[c]
        q_scale = ss[c] * (math.log2(math.e) / math.sqrt(HEAD))
        for h in range(4):
            lanes = slice(h * HEAD, (h + 1) * HEAD)
            y = (acc_q[c, 0, :, lanes] + part_q[c, :, lanes]) * q_scale
            q[c, h] = turn(y, cosine, sine).astype(bf16)

    def each(first, last, body):
        def one(i, unused):
            body(i)
            return unused

        lax.fori_loop(first, last, one, 0)

    def when(i, n, action):
        pl.when(i == n)(action)

    def landed(c, first, last):
        for b in KEY_ORDER[first:last]:
            kv.from_core(c, b)

    def unit(qc, kc, start, stop, first, last, between=()):
        q_block = order[2 * cp + qc]
        which, slots = {}, {}
        for p in range(start, stop):
            slots[p] = kv_slot(KEY_ORDER[p])
            k_block = order[2 * slots[p] + kc]
            which[p] = jnp.where(k_block < q_block, 0, jnp.where(k_block == q_block, 1, 2))
        group = 4
        tops = {}

        def score(h, p, best):
            scr = (scr_a, scr_b)[h % 2]
            halves = [kvg[kc, 0, slots[p], :HALF], kvg[kc, 0, slots[p], HALF:]]
            keys = jnp.concatenate(halves, axis=1)
            scores = jnp.dot(q[qc, h], keys, preferred_element_type=f32) + bias[which[p]]
            scr[:, p * ROWS : (p + 1) * ROWS] = scores
            here = jnp.maximum(scores[:, :HEAD], scores[:, HEAD:])
            return here if best is None else jnp.maximum(best, here)

        def settle(h, best):
            new_top = jnp.broadcast_to(jnp.max(best, axis=1, keepdims=True), (ROWS, HEAD))
            tops[h] = new_top if first else jnp.maximum(top[qc, h], new_top)

        def weigh(h, p, total):
            scr = (scr_a, scr_b)[h % 2]
            both = jnp.concatenate([tops[h]] * 2, axis=1)
            weights = [
                jnp.exp2(scr[:, n * ROWS : (n + 1) * ROWS] - both).astype(bf16)
                for n in range(p, p + group)
            ]
            values = jnp.concatenate([kvg[kc, 1, slots[n]] for n in range(p, p + group)], axis=0)
            here = jnp.dot(
                jnp.concatenate(weights, axis=1),
                jnp.concatenate([values, jnp.ones((group * ROWS, HEAD), bf16)], axis=1),
                preferred_element_type=f32,
            )
            return here if total is None else total + here

        def close(h, total):
            if not first:
                shrink = jnp.exp2(top[qc, h] - tops[h])
                total = total + outs[qc, h] * jnp.concatenate([shrink, shrink], axis=1)
            if last:
                sums = total[:, HEAD:]
                att[qc, 0, h] = (total[:, :HEAD] / sums).astype(bf16)
                att_copy(qc, h).start()
                normalizer = (tops[h] + jnp.log2(sums)) * LN2
                norm_out[h : h + 1, qc * ROWS : (qc + 1) * ROWS] = normalizer.T[:1]
            else:
                top[qc, h] = tops[h]
                outs[qc, h] = total

        best = None
        for p in range(start, stop):
            best = score(0, p, best)
        settle(0, best)
        for h in range(4):
            best = total = None
            for p in range(start, stop):
                if h < 3:
                    best = score(h + 1, p, best)
                if p % group == group - 1:
                    total = weigh(h, p - group + 1, total)
            close(h, total)
            if h < 3:
                settle(h + 1, best)
            if h < len(between) and between[h] is not None:
                between[h]()

    def att_copy(c, h):
        return pltpu.make_async_remote_copy(
            src_ref=att.at[c, 0, h],
            dst_ref=att.at[c, 1, h],
            send_sem=ps.at[c * 4 + h],
            recv_sem=pr.at[c * 4 + h],
            device_id=other,
            device_id_type=MESH,
        )

    def rs_copy(c, n, src, dst, device):
        return pltpu.make_async_remote_copy(
            src_ref=src,
            dst_ref=dst,
            send_sem=rs.at[c * 10 + n],
            recv_sem=rr.at[c * 10 + n],
            device_id=device,
            device_id_type=MESH,
        )

    lo, hi = pl.ds(0, HALF), pl.ds(HALF, HALF)
    ways = (right, left)

    def far_pair(c):
        rs_copy(c, 0, terms.at[c, 2], re.at[c], pair).start()

    def far_out(c):
        block = terms.at[c, 5]
        rs_copy(c, 0, re.at[c], re.at[c], pair).wait_recv()
        block[...] = (block[...].astype(f32) + re[c].astype(f32)).astype(bf16)
        rs_copy(c, 1, block.at[lo], ra.at[c], right).start()
        rs_copy(c, 2, block.at[hi], rb.at[c], left).start()

    def near_pair(c, side):
        rs_copy(c, 3 + side, terms.at[c, side], (rc, rd)[side].at[c, 1], ways[side]).start()

    def near_free(c, side):
        half = (hi, lo)[side]
        rs_copy(
            c, 5 + side, terms.at[c, 3 + side].at[half], (rc, rd)[side].at[c, 0].at[half], ways[side]
        ).start()

    def near_joined(c, side):
        half = (lo, hi)[side]
        block, moved = terms.at[c, 3 + side].at[half], (ra, rb)[side].at[c]
        rs_copy(c, 1 + side, moved, moved, left).wait_recv()
        block[...] = (block[...].astype(f32) + moved[...].astype(f32)).astype(bf16)
        rs_copy(c, 7 + side, block, (rc, rd)[side].at[c, 0].at[half], ways[side]).start()

    def here_in(c, p):
        term = terms[c, 7 - p].astype(f32)
        for side in range(2):
            block = (rc, rd)[side].at[c, p]
            if p == 1:
                rs_copy(c, 3 + side, block, block, left).wait_recv()
            else:
                for n, half in ((5, (hi, lo)[side]), (7, (lo, hi)[side])):
                    rs_copy(c, n + side, block.at[half], block.at[half], left).wait_recv()
            term = term + block[...].astype(f32)
        if p == 1:
            block = terms.at[c, 6]
            block[...] = term.astype(bf16)
            rs_copy(c, 9, block, ry.at[c], pair).start()
        else:
            rs_copy(c, 9, ry.at[c], ry.at[c], pair).wait_recv()
            proj[c * ROWS : (c + 1) * ROWS] = (term + ry[c].astype(f32)).astype(bf16)

    def rs_drain(c):
        whole, half = terms.at[c, 0], terms.at[c, 0, lo]
        for n in range(10):
            ref = half if n in (1, 2, 5, 6, 7, 8) else whole
            rs_copy(c, n, ref, ref, other).wait_send()
        for h in range(4):
            att_copy(c, h).wait_send()

    block_of = {dest: b for b, dest in enumerate((RING[n % 4], n // 4) for n in range(8))}

    def out_products(c):
        def partner():
            for h in range(4):
                att_copy(c, h).wait_recv()

        events = {
            0: lambda: near_pair(c, 0),
            1: lambda: near_pair(c, 1),
            2: lambda: far_pair(c),
        }
        if c == 0:
            events[3] = lambda: near_free(c, 0)
            events[4] = lambda: near_free(c, 1)

        def one(i):
            b = pick(i, [block_of[dest] for dest in DESTS])
            term = None
            for owner in range(2):
                rows = jnp.concatenate([att[c, owner, h] for h in range(4)], axis=1)
                here = jnp.dot(rows, wo[owner, b], preferred_element_type=f32)
                if term is None:
                    when(i, 0, partner)
                term = here if term is None else term + here
            terms[c, i] = term.astype(bf16)
            for n, action in events.items():
                when(i, n, action)

        each(0, 8, one)

    def gather_event(n):
        if n == 2:
            g.from_sides(0)
        if n == 4:
            g.from_pair(0)
            g.pass_pair(0)
        if n == 5:
            g.from_far(0)
        if n == 6:
            g.pass_on(1)
            g.start_second(1)
            g.from_pair(1)
            g.pass_pair(1)
        if n == 7:
            g.from_last(0)
        if n == 8:
            g.from_pair_sides(0)
        if n == 11:
            kv.pass_on(0)
            g.from_sides(1)
        if n == 13:
            kv.from_sides(0)
            kv.from_pair(0)
            kv.pass_pair(0)
            kv.from_far(0)
            kv.from_pair_sides(0)
            g.from_last(1)

    def steps(first, last):
        def one(i):
            for n in (2, 4, 5, 6, 7, 8, 11, 13):
                if first <= n < last:
                    when(i, n, functools.partial(gather_event, n))
            code = pick(i - first, [c * 8 + b for c, b in PLAN[first:last]])
            c, b = code // 8, code % 8

            def ready():
                wq_copy(b).wait()
                wq_across(b).wait_recv()

            if any(c == 0 for c, b in PLAN[first:last]):
                pl.when(c == 0)(ready)
            project(c, b)

        each(first, last, one)

    g.pass_on(0)
    g.start_first(1)
    wk_copy.wait()
    wv_copy.wait()
    wk_across.wait_recv()
    wv_across.wait_recv()
    steps(0, 10)
    send_partials(0)
    partial_copy(0, 1).start()
    finish_kv(0)
    g.from_far(1)
    finish_q(0)
    steps(10, 14)
    kv.from_last(0)
    landed(0, 0, 4)
    g.from_pair_sides(1)
    late = [scaled_block(1, b) for b in (5, 6)]
    for b, (wide, scaled) in zip((5, 6), late):
        project_kv(1, b, wide, scaled)
    send_partials(1)
    for b, (wide, scaled) in zip((5, 6), late):
        project_q(1, b, scaled)
    partial_copy(1, 1).start()
    finish_kv(1)
    landed(0, 4, 8)
    finish_q(1)
    g.drain(0)
    g.drain(1)

    def near_keys():
        kv.from_sides(1)
        kv.from_pair(1)
        kv.pass_pair(1)

    unit(0, 0, 0, 8, True, False, (lambda: kv.pass_on(1), near_keys))
    kv.from_far(1)
    landed(1, 0, 4)
    unit(0, 1, 0, 4, False, False, (None, None, lambda: kv.from_pair_sides(1)))
    kv.from_last(1)
    landed(1, 4, 8)
    unit(0, 1, 4, 8, False, True)
    for b in range(8):
        wo_copy(b).wait()
        wo_across(b).wait_recv()
    out_products(0)
    unit(1, 0, 0, 8, True, False)
    unit(1, 1, 0, 4, False, False)
    unit(1, 1, 4, 8, False, True, (lambda: far_out(0),))
    out_products(1)
    here_in(0, 1)
    near_joined(0, 0)
    near_joined(0, 1)
    far_out(1)
    near_free(1, 0)
    near_free(1, 1)
    here_in(1, 1)
    here_in(0, 0)
    near_joined(1, 0)
    near_joined(1, 1)
    for b in range(8):
        wq_across(b).wait_send()
        wo_across(b).wait_send()
    wk_across.wait_send()
    wv_across.wait_send()
    for c in range(2):
        partial_copy(c, 0).wait_send()
        partial_copy(c, 1).wait_send()
        kv.drain(c)
    rs_drain(0)
    here_in(1, 0)
    rs_drain(1)


def hand_over(proj, norm, proj_out, norm_out):
    proj_out[...] = proj[...]
    norm_out[...] = norm[...]


def shards(
    checkpoint, norm_gain, query_weight, key_weight, value_weight, output_weight, block_order
):
    vmem = pl.BlockSpec(memory_space=pltpu.VMEM)
    hbm = pl.BlockSpec(memory_space=pl.ANY)
    dma = pltpu.SemaphoreType.DMA
    shapes = (
        jax.ShapeDtypeStruct((2 * ROWS, FEAT), bf16),
        jax.ShapeDtypeStruct((4, 2 * ROWS), f32),
    )
    results = pl.pallas_call(
        kernel,
        out_shape=tuple(pltpu.VMEM(shape.shape, shape.dtype) for shape in shapes),
        in_specs=[pl.BlockSpec(memory_space=pltpu.SMEM), hbm, vmem, hbm, hbm, hbm, hbm],
        out_specs=(vmem, vmem),
        scratch_shapes=[
            pltpu.VMEM((2, 8, ROWS, FEAT), bf16),
            pltpu.VMEM((2, 8, FEAT, FEAT), bf16),
            pltpu.VMEM((2 * HEAD, D), bf16),
            pltpu.VMEM((2, 8, FEAT, FEAT), bf16),
            pltpu.VMEM((2, 2, ROWS, FEAT), f32),
            pltpu.VMEM((2, ROWS, 2 * HEAD), f32),
            pltpu.VMEM((2, ROWS, HEAD), f32),
            pltpu.VMEM((2, ROWS, 2 * HEAD), f32),
            pltpu.VMEM((2, ROWS, FEAT), f32),
            pltpu.VMEM((2, ROWS, 2 * HEAD), f32),
            pltpu.VMEM((2, ROWS, HEAD), f32),
            pltpu.VMEM((2, ROWS, HEAD), f32),
            pltpu.VMEM((2, 4, ROWS, HEAD), bf16),
            pltpu.VMEM((2, 2, N_CP, ROWS, HEAD), bf16),
            pltpu.VMEM((ROWS, N_CP * ROWS), f32),
            pltpu.VMEM((ROWS, N_CP * ROWS), f32),
            pltpu.VMEM((2, 4, ROWS, HEAD), f32),
            pltpu.VMEM((2, 4, ROWS, 2 * HEAD), f32),
            pltpu.VMEM((2, 2, 4, ROWS, HEAD), bf16),
            pltpu.VMEM((3, ROWS, ROWS), f32),
            pltpu.VMEM((2, 8, ROWS, FEAT), bf16),
            pltpu.VMEM((2, HALF, FEAT), bf16),
            pltpu.VMEM((2, HALF, FEAT), bf16),
            pltpu.VMEM((2, 2, ROWS, FEAT), bf16),
            pltpu.VMEM((2, 2, ROWS, FEAT), bf16),
            pltpu.VMEM((2, ROWS, FEAT), bf16),
            pltpu.VMEM((2, ROWS, FEAT), bf16),
            dma((2,)),
            dma((18,)),
            dma((22,)),
            dma((22,)),
            dma((20,)),
            dma((20,)),
            dma((36,)),
            dma((36,)),
            dma((8,)),
            dma((8,)),
            dma((20,)),
            dma((20,)),
        ],
        compiler_params=pltpu.CompilerParams(
            collective_id=0, has_side_effects=True, vmem_limit_bytes=63000000
        ),
        name="sublayer",
    )(
        block_order,
        checkpoint,
        norm_gain.reshape(D // HEAD, HEAD),
        query_weight,
        key_weight.T,
        value_weight.T,
        output_weight,
    )
    return pl.pallas_call(
        hand_over,
        out_shape=shapes,
        in_specs=[vmem, vmem],
        out_specs=(vmem, vmem),
        name="hand_over",
    )(*(pltpu.with_memory_space_constraint(result, pltpu.VMEM) for result in results))


def solution(mesh):
    return jax.shard_map(
        shards,
        mesh=mesh,
        in_specs=(
            P("cp", "tp"),
            P(),
            P(None, "tp"),
            P(None, "tp"),
            P(None, "tp"),
            P("tp", None),
            P(),
        ),
        out_specs=(P("cp", "tp"), P("tp", "cp")),
        check_vma=False,
    )
```
